256 devices in a mesh: px: 32 (over y, z_hi, core), py: 8 (over z_lo, x).
Axes of the slice: x: 4, y: 4, z: 8 (z_hi: 4, z_lo: 2; z = z_hi * 2 + z_lo), core: 2. Of those that a mesh axis runs over, the one named last changes fastest.
Arguments:
- charges_old: float32 [32, 8, 32, 32, 512], P('px', 'py'), may hold values from -0.0026758191 to 0.0026758191
- spline_moduli: float32 [3, 512], replicated, may hold values from 1 to 2.5
Outputs:
- structure: float32 [2, 512, 512, 512], P(None, 'px', 'py')
- energy: float32 [], replicated
- virial: float32 [6], replicated
The draws below stay inside these ranges and needn't reach their ends.
All inputs are finite; a program needn't handle non-finite values.
Results may differ from the reference program's by a relative error of at most 0.0007.
Values sent between devices are 32-bit elements; how exact they have to be, the bound alone decides.
A program may use at most 128 MiB of HBM per device.

```python
import math
import jax
import jax.numpy as jnp
from jax import lax

GRID = 512
PENCIL_ROWS = 32
PENCIL_COLS = 8
OLD_BX = 32
OLD_BY = 32


def draw_charges_old(key, part):
    key_list = jax.random.split(key, 3)
    full_shape = (PENCIL_ROWS, PENCIL_COLS, OLD_BX, OLD_BY, GRID)
    log_ten = math.log(10.0)
    row_scale = jnp.exp(jax.random.uniform(key_list[0], (GRID,), jnp.float32) * log_ten)
    col_scale = jnp.exp(jax.random.uniform(key_list[1], (GRID,), jnp.float32) * log_ten)
    pencil_row = jnp.arange(PENCIL_ROWS, dtype=jnp.int32).reshape(PENCIL_ROWS, 1, 1, 1, 1)
    pencil_col = jnp.arange(PENCIL_COLS, dtype=jnp.int32).reshape(1, PENCIL_COLS, 1, 1, 1)
    inner_row = jnp.arange(OLD_BX, dtype=jnp.int32).reshape(1, 1, OLD_BX, 1, 1)
    inner_col = jnp.arange(OLD_BY, dtype=jnp.int32).reshape(1, 1, 1, OLD_BY, 1)
    x_position = pencil_row // 2 * OLD_BX + inner_row
    y_position = (pencil_row % 2 * PENCIL_COLS + pencil_col) * OLD_BY + inner_col
    noise_field = jnp.clip(jax.random.normal(key_list[2], full_shape, jnp.float32), -6.0, 6.0)
    values = noise_field * row_scale[x_position] * col_scale[y_position]
    return values / (20.0 * GRID ** 1.5)


def setup_inputs(seed: int = 0) -> dict:
    streams_of = jax.random.split(jax.random.key(seed), 3)
    return {
        "charges_old": draw_charges_old(jax.random.fold_in(streams_of[2], 71), 0),
        "spline_moduli": jnp.clip(jnp.exp(jax.random.uniform(streams_of[1], (3, GRID), jnp.float32, math.log(1.0), math.log(2.5))), 1.0, 2.5),
    }


beta_nm = 3.12
cell_nm = 0.1


def signed_wave(mode_index, points):
    shifted = mode_index - points * (mode_index >= points // 2).astype(jnp.int32)
    return shifted.astype(jnp.float32) / (cell_nm * points)


def mode_sums(real_part, imag_part, wave_y, wave_z, wave_x, moduli_y, moduli_z, moduli_x, points):
    m_square = wave_y * wave_y + wave_z * wave_z + wave_x * wave_x
    anchor = m_square == 0.0
    safe_msq = jnp.where(anchor, 1.0, m_square)
    volume = (cell_nm * points) ** 3
    decay_ratio = (math.pi ** 2 / beta_nm ** 2) * m_square
    influence = jnp.exp(-decay_ratio) / (math.pi * volume * safe_msq) * moduli_y * moduli_z * moduli_x
    influence = jnp.where(anchor, 0.0, influence)
    mode_power = influence * (real_part * real_part + imag_part * imag_part)
    energy = 0.5 * jnp.sum(mode_power)
    weight = mode_power * (1.0 + decay_ratio) / safe_msq
    pair_sums = jnp.stack([
        jnp.sum(weight * wave_x * wave_x),
        jnp.sum(weight * wave_y * wave_y),
        jnp.sum(weight * wave_z * wave_z),
        jnp.sum(weight * wave_x * wave_y),
        jnp.sum(weight * wave_x * wave_z),
        jnp.sum(weight * wave_y * wave_z),
    ])
    return energy, pair_sums


def reference(charges_old, spline_moduli):
    points = GRID
    blocks = charges_old.reshape(PENCIL_ROWS // 2, 2, PENCIL_COLS, OLD_BX, OLD_BY, points)
    charge_mesh = blocks.transpose(0, 3, 1, 2, 4, 5).reshape(points, points, points)
    spectrum = jnp.transpose(jnp.fft.fftn(charge_mesh), (1, 2, 0))
    real_part = jnp.real(spectrum)
    imag_part = jnp.imag(spectrum)
    mode_index = jnp.arange(points, dtype=jnp.int32)
    wave_numbers = signed_wave(mode_index, points)
    wave_z = wave_numbers[:, None]
    wave_x = wave_numbers[None, :]
    moduli_z = spline_moduli[2][:, None]
    moduli_x = spline_moduli[0][None, :]

    def per_plane(plane_items):
        real_plane, imag_plane, wave_plane, moduli_plane = plane_items
        return mode_sums(real_plane, imag_plane, wave_plane, wave_z, wave_x, moduli_plane, moduli_z, moduli_x, points)

    energies, pair_sums = lax.map(per_plane, (real_part, imag_part, wave_numbers, spline_moduli[1]))
    energy = jnp.sum(energies)
    virial = energy * jnp.array([1.0, 1.0, 1.0, 0.0, 0.0, 0.0], dtype=jnp.float32) - jnp.sum(pair_sums, axis=0)
    structure = jnp.stack([real_part, imag_part])
    return structure, energy, virial
```

```python
import functools
import math

import jax
import jax.numpy as jnp
import numpy as np
from jax import lax
from jax.experimental import pallas as pl
from jax.experimental.pallas import tpu as pltpu
from jax.sharding import Mesh
from jax.sharding import PartitionSpec as P

AXES = ("px_0", "px_1", "px_2", "py_0", "py_1")
PX = AXES[:3]
PY = AXES[3:]
MESH = pl.DeviceIdType.MESH
F32 = jnp.float32
BF16 = jnp.bfloat16

beta_nm = 3.12
cell_nm = 0.1
N = 512
HALF = N // 2
NT = (((1,), (1,)), ((), ()))


def split_np(a):
    hi = a.astype(BF16)
    lo = (a - hi.astype(np.float64)).astype(BF16)
    return np.stack([hi, lo])


def angles(rows, cols):
    return 2.0 * math.pi * (np.outer(rows, cols) % N) / N


def z_table():
    z = np.arange(N)
    parts = []
    for b in range(4):
        t = angles(z, 64 * b + np.arange(64))
        parts += [np.cos(t), -np.sin(t)]
    edge = np.zeros((N, 128))
    for b in range(4):
        t = angles(z, np.array([64 * (b + 1)]))[:, 0]
        edge[:, 8 * b] = np.cos(t)
        edge[:, 64 + 8 * b] = -np.sin(t)
    return split_np(np.concatenate(parts + [edge], axis=1))


def y_table():
    r = np.arange(HALF)
    out = []
    for e in range(2):
        t = angles(2 * np.arange(HALF) + e, r)
        out.append(np.concatenate([np.cos(t), np.sin(t)], axis=1))
    return split_np(np.stack(out))


def x_table():
    r = np.arange(HALF)
    out = []
    for a in range(2):
        t = angles(2 * r + a, np.arange(HALF))
        out.append(np.concatenate([np.cos(t), np.sin(t)], axis=1))
    return split_np(np.stack(out))


def split(v):
    hi = v.astype(BF16)
    return hi, (v - hi.astype(F32)).astype(BF16)


def mm(a, b):
    return jnp.dot(a, b, preferred_element_type=F32)


def exchange_kernel(x_ref, wz_ref, wy_ref, r2_ref, zs, r1, zy, send1, recv1, send2, recv2):
    yc, zh, c, lo, xc = [lax.axis_index(a) for a in AXES]
    p = yc * 8 + zh * 2 + c
    me16 = c * 8 + lo * 4 + xc
    me64 = p * 2 + lo
    b = xc + lo * (3 - 2 * xc)

    def peer16(t):
        d = lax.rem(me16 + t, 16)
        dc = lax.div(d, 8)
        dl = lax.rem(lax.div(d, 4), 2)
        dx = lax.rem(d, 4)
        return dc, dl, dx

    def peer64(t):
        d = lax.rem(me64 + t, 64)
        dp = lax.div(d, 2)
        dl = lax.rem(d, 2)
        dx = b + dl * (3 - 2 * b)
        return dp, dl, dx, (lax.div(dp, 8), lax.rem(lax.div(dp, 2), 4), lax.rem(dp, 2), dl, dx)

    barrier = pltpu.get_barrier_semaphore()

    def greet16(t, carry):
        dc, dl, dx = peer16(t)
        pl.semaphore_signal(barrier, inc=1, device_id=(yc, zh, dc, dl, dx), device_id_type=MESH)
        return carry

    def greet64(t, carry):
        pl.semaphore_signal(barrier, inc=1, device_id=peer64(t)[3], device_id_type=MESH)
        return carry

    lax.fori_loop(1, 16, greet16, 0)
    lax.fori_loop(1, 64, greet64, 0)

    def z_step(g, carry):
        rows = x_ref[lax.div(g, 2), :, lax.rem(g, 2)].reshape(256, N)
        hi, low = split(rows)
        out = mm(hi, wz_ref[0]) + mm(low, wz_ref[0]) + mm(hi, wz_ref[1])
        for k in range(4):
            zs[g, k, 0:8] = out[:, 128 * k : 128 * k + 128].reshape(8, 32, 128)
        edge = out[:, 512:640].reshape(8, 32, 128)
        packed = edge[0]
        for r in range(1, 8):
            packed = packed + pltpu.roll(edge[r], r, 1)
        zs[g, 0, 8] = packed
        for k in range(1, 4):
            zs[g, k, 8] = pltpu.roll(packed, 128 - 8 * k, 1)
        return carry

    lax.fori_loop(0, 4, z_step, 0)
    pl.semaphore_wait(barrier, 78)

    def send_y(t, carry):
        dc, dl, dx = peer16(t)
        pltpu.make_async_remote_copy(
            src_ref=zs.at[2 * dc + dl, dx + dl * (3 - 2 * dx)],
            dst_ref=r1.at[:, pl.ds(pl.multiple_of(me16 * 32, 32), 32), :],
            send_sem=send1,
            recv_sem=recv1,
            device_id=(yc, zh, dc, dl, dx),
            device_id_type=MESH,
        ).start()
        return carry

    lax.fori_loop(1, 16, send_y, 0)
    r1[:, pl.ds(pl.multiple_of(me16 * 32, 32), 32), :] = zs[2 * c + lo, b]
    pltpu.make_async_copy(r1.at[:, pl.ds(0, 480), :], r1.at[:, pl.ds(0, 480), :], recv1).wait()

    lane = lax.broadcasted_iota(jnp.int32, (HALF, 128), 1)
    is_edge = (lane == 0) | (lane == 64)
    turn = jnp.where(lane < 64, 1.0, -1.0).astype(F32)

    for e in range(2):

        def fold(i):
            top = r1[i, pl.ds(0, HALF), :]
            bottom = r1[i, pl.ds(HALF, HALF), :]
            return top + bottom if e == 0 else top - bottom

        for r in range(8):
            direct = fold(r)
            edge = fold(8)
            if r:
                edge = pltpu.roll(edge, 128 - r, 1)
            mirror = jnp.where(is_edge, edge, direct)
            plain = jnp.concatenate([direct, mirror], axis=1)
            turned = jnp.concatenate(
                [pltpu.roll(direct, 64, 1) * turn, pltpu.roll(mirror, 64, 1) * turn], axis=1
            )
            hi, low = split(jnp.concatenate([plain, turned], axis=0))
            out = mm(wy_ref[0, e], hi) + mm(wy_ref[1, e], hi) + mm(wy_ref[0, e], low)
            zy[e, pl.ds(r, HALF, stride=8), :] = out[:, :128]
            zy[e, pl.ds(264 * 8 + r, HALF, stride=8), :] = out[:, 128:]
        if e == 0:
            zy[e, pl.ds(520 * 8, 8), :] = zy[e, pl.ds(264 * 8, 8), :]

        def rows_for(dp, dl):
            start = (1 - dl) * (8 * dp) + dl * (264 + 249 - e - 8 * dp)
            return zy.at[e, pl.ds(pl.multiple_of(start * 8, 8), 64), :]

        pltpu.make_async_copy(rows_for(p, lo), r2_ref.at[e, lo, p], recv2.at[e]).start()

        def send_x(t, carry):
            dp, dl, dx, device = peer64(t)
            pltpu.make_async_remote_copy(
                src_ref=rows_for(dp, dl),
                dst_ref=r2_ref.at[e, lo, p],
                send_sem=send2.at[e],
                recv_sem=recv2.at[e],
                device_id=device,
                device_id_type=MESH,
            ).start()
            return carry

        lax.fori_loop(1, 64, send_x, 0)

    pltpu.make_async_copy(r1.at[:, pl.ds(0, 480), :], r1.at[:, pl.ds(0, 480), :], send1).wait()
    for e in range(2):
        sent = zy.at[e, pl.ds(0, 63 * 64), :]
        pltpu.make_async_copy(sent, sent, send2.at[e]).wait()
        pltpu.make_async_copy(r2_ref.at[e], r2_ref.at[e], recv2.at[e]).wait()


def exchange(charges):
    vmem = pl.BlockSpec(memory_space=pltpu.VMEM)
    wz, wy = jnp.asarray(z_table()), jnp.asarray(y_table())
    return pl.pallas_call(
        exchange_kernel,
        out_shape=jax.ShapeDtypeStruct((2, 2, 32, 64, 128), F32),
        in_specs=[vmem] * 3,
        out_specs=pl.BlockSpec(memory_space=pl.ANY),
        scratch_shapes=[
            pltpu.VMEM((4, 4, 9, 32, 128), F32),
            pltpu.VMEM((9, N, 128), F32),
            pltpu.VMEM((2, 528 * 8, 128), F32),
            pltpu.SemaphoreType.DMA,
            pltpu.SemaphoreType.DMA,
            pltpu.SemaphoreType.DMA((2,)),
            pltpu.SemaphoreType.DMA((2,)),
        ],
        compiler_params=pltpu.CompilerParams(
            collective_id=0, has_side_effects=True, vmem_limit_bytes=48 * 2**20
        ),
        name="exchange",
    )(charges.reshape(2, 8, 2, 32, N), wz, wy)


GROUP = 2


def finish_kernel(
    flag_ref, yrow_ref, d_ref, wx_ref, wavex_ref, modx_ref, zcol_ref, out_ref, sums_ref, acc, xz2, modxz
):
    e, step = pl.program_id(0), pl.program_id(1)
    flip = flag_ref[0]

    @pl.when((e == 0) & (step == 0))
    def _():
        acc[...] = jnp.zeros_like(acc)
        mx = wavex_ref[...]
        mz = zcol_ref[:, 0:1]
        xz2[...] = mx * mx + mz * mz
        modxz[...] = modx_ref[...] * zcol_ref[:, 1:2] * (1.0 / (math.pi * (cell_nm * N) ** 3))

    row = lax.broadcasted_iota(jnp.int32, (128, 128), 0)
    col = lax.broadcasted_iota(jnp.int32, (128, 128), 1)
    upper = row >= 64
    within = jnp.where(upper, row - 64, row)
    negated = jnp.where(within == 0, 0, 64 - within)
    target = jnp.where(flip == 1, negated, within) + jnp.where(upper, 64, 0)
    sign = jnp.where((flip == 1) & upper, -1.0, 1.0)
    select = jnp.where(col == target, sign, 0.0).astype(BF16)

    def turned(a):
        his, lows = [], []
        for j in range(GROUP):
            slot = jnp.where(flip == 1, GROUP - 1 - j, j)
            hi, low = split(d_ref[0, a, :, slot].reshape(HALF, 128))
            his.append(lax.dot_general(select, hi, NT, preferred_element_type=F32).astype(BF16))
            lows.append(lax.dot_general(select, low, NT, preferred_element_type=F32).astype(BF16))
        hi, low = jnp.concatenate(his, axis=0), jnp.concatenate(lows, axis=0)
        return mm(hi, wx_ref[0, a]) + mm(low, wx_ref[0, a]) + mm(hi, wx_ref[1, a])

    even, odd = turned(0), turned(1)
    mz = zcol_ref[:, 0:1]
    for j in range(GROUP):

        def parts(v):
            re, im = v[128 * j : 128 * j + 64], v[128 * j + 64 : 128 * j + 128]
            return re[:, :HALF] + im[:, HALF:], im[:, :HALF] - re[:, HALF:]

        er, ei = parts(even)
        orr, oi = parts(odd)
        re = jnp.concatenate([er + orr, er - orr], axis=1)
        im = jnp.concatenate([ei + oi, ei - oi], axis=1)
        out_ref[0, j, 0] = re
        out_ref[1, j, 0] = im
        index = 2 * (GROUP * step + j) + e
        my, mody = yrow_ref[0, index], yrow_ref[1, index]
        msq = xz2[...] + my * my
        anchor = msq == 0.0
        inverse = 1.0 / jnp.where(anchor, 1.0, msq)
        decay = (math.pi**2 / beta_nm**2) * msq
        theta = jnp.where(anchor, 0.0, jnp.exp(-decay) * inverse * modxz[...] * mody)
        power = theta * (re * re + im * im)
        weight = power * (1.0 + decay) * inverse

        def rows(v):
            return jnp.sum(v.reshape(8, 8, N), axis=0)

        wz = weight * mz
        w0, w1, w2 = rows(weight), rows(wz), rows(wz * mz)
        acc[0] += rows(power)
        acc[1] += w0
        acc[2] += w0 * (my * my)
        acc[3] += w2
        acc[4] += w0 * my
        acc[5] += w1
        acc[6] += w1 * my

    @pl.when((e == 1) & (step == pl.num_programs(1) - 1))
    def _():
        mx = wavex_ref[...]

        def lanes(v):
            v = jnp.sum(v, axis=0, keepdims=True)
            return v[:, 0:128] + v[:, 128:256] + v[:, 256:384] + v[:, 384:512]

        sums_ref[...] = jnp.concatenate(
            [
                lanes(acc[0]),
                lanes(acc[1] * (mx * mx)),
                lanes(acc[2]),
                lanes(acc[3]),
                lanes(acc[4] * mx),
                lanes(acc[5] * mx),
                lanes(acc[6]),
                jnp.zeros((1, 128), F32),
            ],
            axis=0,
        )


def finish(gathered, flip, yrow, wavex, modx, zcol):
    wx = jnp.asarray(x_table())
    steps = 8 // GROUP

    def whole(shape):
        return pl.BlockSpec(shape, lambda e, s, flag: (0,) * len(shape))

    return pl.pallas_call(
        finish_kernel,
        out_shape=(
            jax.ShapeDtypeStruct((2, 8, 2, 64, N), F32),
            jax.ShapeDtypeStruct((8, 128), F32),
        ),
        grid_spec=pltpu.PrefetchScalarGridSpec(
            num_scalar_prefetch=1,
            grid=(2, steps),
            in_specs=[
                pl.BlockSpec(memory_space=pltpu.SMEM),
                pl.BlockSpec(
                    (1, 2, 32, GROUP, 8, 128),
                    lambda e, s, flag: (e, 0, 0, s + flag[0] * (steps - 1 - 2 * s), 0, 0),
                ),
                whole((2, 2, HALF, N)),
                whole((1, N)),
                whole((1, N)),
                whole((64, 128)),
            ],
            out_specs=[
                pl.BlockSpec((2, GROUP, 1, 64, N), lambda e, s, flag: (0, s, e, 0, 0)),
                whole((8, 128)),
            ],
            scratch_shapes=[
                pltpu.VMEM((7, 8, N), F32),
                pltpu.VMEM((64, N), F32),
                pltpu.VMEM((64, N), F32),
            ],
        ),
        compiler_params=pltpu.CompilerParams(vmem_limit_bytes=40 * 2**20),
        name="finish",
    )(flip, yrow, gathered, wx, wavex, modx, zcol)


def signed_wave(mode_index):
    shifted = mode_index - N * (mode_index >= HALF).astype(jnp.int32)
    return shifted.astype(F32) / (cell_nm * N)


def body(charges_old, spline_moduli):
    row = lax.axis_index(PX)
    col = lax.axis_index(PY)
    lo = lax.axis_index("py_0")
    ky = row * 16 + jnp.arange(16, dtype=jnp.int32)
    kz = col * 64 + jnp.arange(64, dtype=jnp.int32)
    kx = jnp.arange(N, dtype=jnp.int32)
    mody = lax.dynamic_slice_in_dim(spline_moduli[1], row * 16, 16)
    modz = lax.dynamic_slice_in_dim(spline_moduli[2], col * 64, 64)
    yrow = jnp.stack([signed_wave(ky), mody])
    pick = jnp.arange(128, dtype=jnp.int32)[None, :]
    zcol = jnp.where(pick == 0, signed_wave(kz)[:, None], modz[:, None])
    wavex = signed_wave(kx)[None, :]
    modx = spline_moduli[0][None, :]

    gathered = exchange(charges_old).reshape(2, 2, 32, 8, 8, 128)
    structure, sums = finish(gathered, lo.astype(jnp.int32).reshape(1), yrow, wavex, modx, zcol)
    totals = lax.psum(jnp.sum(sums, axis=1), AXES)
    energy = 0.5 * totals[0]
    virial = energy * jnp.array([1.0, 1.0, 1.0, 0.0, 0.0, 0.0], dtype=F32) - totals[1:7]
    return structure.reshape(2, 16, 64, N), energy, virial


def solution(mesh):
    torus = Mesh(mesh.devices.reshape(4, 4, 2, 2, 4), AXES)
    return jax.shard_map(
        body,
        mesh=torus,
        in_specs=(P(PX, PY, None, None, None), P()),
        out_specs=(P(None, PX, PY, None), P(), P()),
        check_vma=False,
    )
```

```python
import functools
import math

import jax
import jax.numpy as jnp
import numpy as np
from jax import lax
from jax.experimental import pallas as pl
from jax.experimental.pallas import tpu as pltpu
from jax.sharding import Mesh
from jax.sharding import PartitionSpec as P

AXES = ("px_0", "px_1", "px_2", "py_0", "py_1")
PX = AXES[:3]
PY = AXES[3:]
MESH = pl.DeviceIdType.MESH
F32 = jnp.float32
BF16 = jnp.bfloat16

beta_nm = 3.12
cell_nm = 0.1
N = 512
HALF = N // 2
NT = (((1,), (1,)), ((), ()))


def split_np(a):
    hi = a.astype(BF16)
    lo = (a - hi.astype(np.float64)).astype(BF16)
    return np.stack([hi, lo])


def angles(rows, cols):
    return 2.0 * math.pi * (np.outer(rows, cols) % N) / N


def z_table():
    z = np.arange(N)
    parts = []
    for b in range(4):
        t = angles(z, 64 * b + np.arange(64))
        parts += [np.cos(t), -np.sin(t)]
    edge = np.zeros((N, 128))
    for b in range(4):
        t = angles(z, np.array([64 * (b + 1)]))[:, 0]
        edge[:, 8 * b] = np.cos(t)
        edge[:, 64 + 8 * b] = -np.sin(t)
    return split_np(np.concatenate(parts + [edge], axis=1))


def y_table():
    r = np.arange(HALF)
    out = []
    for e in range(2):
        t = angles(2 * np.arange(HALF) + e, r)
        out.append(np.concatenate([np.cos(t), np.sin(t)], axis=1))
    return split_np(np.stack(out))


def x_table():
    r = np.arange(HALF)
    out = []
    for a in range(2):
        t = angles(2 * r + a, np.arange(HALF))
        out.append(np.concatenate([np.cos(t), np.sin(t)], axis=1))
    return split_np(np.stack(out))


def split(v):
    hi = v.astype(BF16)
    return hi, (v - hi.astype(F32)).astype(BF16)


def mm(a, b):
    return jnp.dot(a, b, preferred_element_type=F32)


def exchange_kernel(
    x_hbm, wz_hbm, wy_hbm, r2_ref, x_ref, wz_ref, wy_ref, zs, r1, zy, load, send1, recv1, send2, recv2
):
    loads = [
        pltpu.make_async_copy(source, target, load.at[i])
        for i, (source, target) in enumerate(((x_hbm, x_ref), (wz_hbm, wz_ref), (wy_hbm, wy_ref)))
    ]
    for copy in loads:
        copy.start()
    yc, zh, c, lo, xc = [lax.axis_index(a) for a in AXES]
    p = yc * 8 + zh * 2 + c
    me16 = c * 8 + lo * 4 + xc
    me64 = p * 2 + lo
    b = xc + lo * (3 - 2 * xc)

    def peer16(t):
        d = lax.rem(me16 + t, 16)
        dc = lax.div(d, 8)
        dl = lax.rem(lax.div(d, 4), 2)
        dx = lax.rem(d, 4)
        return dc, dl, dx

    def peer64(t):
        d = lax.rem(me64 + t, 64)
        dp = lax.div(d, 2)
        dl = lax.rem(d, 2)
        dx = b + dl * (3 - 2 * b)
        return dp, dl, dx, (lax.div(dp, 8), lax.rem(lax.div(dp, 2), 4), lax.rem(dp, 2), dl, dx)

    barrier = pltpu.get_barrier_semaphore()

    def greet16(t, carry):
        dc, dl, dx = peer16(t)
        pl.semaphore_signal(barrier, inc=1, device_id=(yc, zh, dc, dl, dx), device_id_type=MESH)
        return carry

    def greet64(t, carry):
        pl.semaphore_signal(barrier, inc=1, device_id=peer64(t)[3], device_id_type=MESH)
        return carry

    lax.fori_loop(1, 16, greet16, 0)
    lax.fori_loop(1, 64, greet64, 0)

    def z_step(g, carry):
        rows = x_ref[lax.div(g, 2), :, lax.rem(g, 2)].reshape(256, N)
        hi, low = split(rows)
        out = mm(hi, wz_ref[0]) + mm(low, wz_ref[0]) + mm(hi, wz_ref[1])
        for k in range(4):
            zs[g, k, 0:8] = out[:, 128 * k : 128 * k + 128].reshape(8, 32, 128)
        edge = out[:, 512:640].reshape(8, 32, 128)
        packed = edge[0]
        for r in range(1, 8):
            packed = packed + pltpu.roll(edge[r], r, 1)
        zs[g, 0, 8] = packed
        for k in range(1, 4):
            zs[g, k, 8] = pltpu.roll(packed, 128 - 8 * k, 1)
        return carry

    loads[0].wait()
    loads[1].wait()
    lax.fori_loop(0, 4, z_step, 0)
    pl.semaphore_wait(barrier, 78)

    def send_y(t, carry):
        dc, dl, dx = peer16(t)
        pltpu.make_async_remote_copy(
            src_ref=zs.at[2 * dc + dl, dx + dl * (3 - 2 * dx)],
            dst_ref=r1.at[:, pl.ds(pl.multiple_of(me16 * 32, 32), 32), :],
            send_sem=send1,
            recv_sem=recv1,
            device_id=(yc, zh, dc, dl, dx),
            device_id_type=MESH,
        ).start()
        return carry

    lax.fori_loop(1, 16, send_y, 0)
    r1[:, pl.ds(pl.multiple_of(me16 * 32, 32), 32), :] = zs[2 * c + lo, b]
    pltpu.make_async_copy(r1.at[:, pl.ds(0, 480), :], r1.at[:, pl.ds(0, 480), :], recv1).wait()

    loads[2].wait()
    lane = lax.broadcasted_iota(jnp.int32, (HALF, 128), 1)
    is_edge = (lane == 0) | (lane == 64)
    turn = jnp.where(lane < 64, 1.0, -1.0).astype(F32)

    for e in range(2):

        def fold(i):
            top = r1[i, pl.ds(0, HALF), :]
            bottom = r1[i, pl.ds(HALF, HALF), :]
            return top + bottom if e == 0 else top - bottom

        for r in range(8):
            direct = fold(r)
            edge = fold(8)
            if r:
                edge = pltpu.roll(edge, 128 - r, 1)
            mirror = jnp.where(is_edge, edge, direct)
            plain = jnp.concatenate([direct, mirror], axis=1)
            turned = jnp.concatenate(
                [pltpu.roll(direct, 64, 1) * turn, pltpu.roll(mirror, 64, 1) * turn], axis=1
            )
            hi, low = split(jnp.concatenate([plain, turned], axis=0))
            out = mm(wy_ref[0, e], hi) + mm(wy_ref[1, e], hi) + mm(wy_ref[0, e], low)
            zy[e, pl.ds(r, HALF, stride=8), :] = out[:, :128]
            zy[e, pl.ds(264 * 8 + r, HALF, stride=8), :] = out[:, 128:]
        if e == 0:
            zy[e, pl.ds(520 * 8, 8), :] = zy[e, pl.ds(264 * 8, 8), :]

        def rows_for(dp, dl):
            start = (1 - dl) * (8 * dp) + dl * (264 + 249 - e - 8 * dp)
            return zy.at[e, pl.ds(pl.multiple_of(start * 8, 8), 64), :]

        pltpu.make_async_copy(rows_for(p, lo), r2_ref.at[e, lo, p], recv2.at[e]).start()

        def send_x(t, carry):
            dp, dl, dx, device = peer64(t)
            pltpu.make_async_remote_copy(
                src_ref=rows_for(dp, dl),
                dst_ref=r2_ref.at[e, lo, p],
                send_sem=send2.at[e],
                recv_sem=recv2.at[e],
                device_id=device,
                device_id_type=MESH,
            ).start()
            return carry

        lax.fori_loop(1, 64, send_x, 0)

    pltpu.make_async_copy(r1.at[:, pl.ds(0, 480), :], r1.at[:, pl.ds(0, 480), :], send1).wait()
    for e in range(2):
        sent = zy.at[e, pl.ds(0, 63 * 64), :]
        pltpu.make_async_copy(sent, sent, send2.at[e]).wait()
        pltpu.make_async_copy(r2_ref.at[e], r2_ref.at[e], recv2.at[e]).wait()


def exchange(charges):
    wz, wy = jnp.asarray(z_table()), jnp.asarray(y_table())
    return pl.pallas_call(
        exchange_kernel,
        out_shape=jax.ShapeDtypeStruct((2, 2, 32, 64, 128), F32),
        in_specs=[pl.BlockSpec(memory_space=pl.ANY)] * 3,
        out_specs=pl.BlockSpec(memory_space=pl.ANY),
        scratch_shapes=[
            pltpu.VMEM((2, 8, 2, 32, N), F32),
            pltpu.VMEM((2, N, 640), BF16),
            pltpu.VMEM((2, 2, HALF, N), BF16),
            pltpu.VMEM((4, 4, 9, 32, 128), F32),
            pltpu.VMEM((9, N, 128), F32),
            pltpu.VMEM((2, 528 * 8, 128), F32),
            pltpu.SemaphoreType.DMA((3,)),
            pltpu.SemaphoreType.DMA,
            pltpu.SemaphoreType.DMA,
            pltpu.SemaphoreType.DMA((2,)),
            pltpu.SemaphoreType.DMA((2,)),
        ],
        compiler_params=pltpu.CompilerParams(
            collective_id=0, has_side_effects=True, vmem_limit_bytes=62 * 2**20
        ),
        name="exchange",
    )(charges.reshape(2, 8, 2, 32, N), wz, wy)


GROUP = 2


def signed_wave(mode_index):
    shifted = mode_index - N * (mode_index >= HALF).astype(jnp.int32)
    return shifted.astype(F32) / (cell_nm * N)


def finish_kernel(place_ref, mod_smem, d_ref, wx_ref, mod_ref, out_ref, sums_ref, acc, xz2, modxz):
    e, step = pl.program_id(0), pl.program_id(1)
    flip, px, py = place_ref[0], place_ref[1], place_ref[2]
    mx = signed_wave(lax.broadcasted_iota(jnp.int32, (1, N), 1))
    mz = signed_wave(64 * py + lax.broadcasted_iota(jnp.int32, (64, 1), 0))

    @pl.when((e == 0) & (step == 0))
    def _():
        acc[...] = jnp.zeros_like(acc)
        xz2[...] = mx * mx + mz * mz
        modz = pltpu.roll(jnp.broadcast_to(mod_ref[2:3, :], (8, N)), lax.rem(N - 64 * py, N), 1)
        modz = jnp.broadcast_to(modz[0:1, :128], (128, 128)).T[:64]
        modz = jnp.concatenate([modz] * 4, axis=1)
        modxz[...] = mod_ref[0:1, :] * modz * (1.0 / (math.pi * (cell_nm * N) ** 3))

    row = lax.broadcasted_iota(jnp.int32, (128, 128), 0)
    col = lax.broadcasted_iota(jnp.int32, (128, 128), 1)
    upper = row >= 64
    within = jnp.where(upper, row - 64, row)
    negated = jnp.where(within == 0, 0, 64 - within)
    target = jnp.where(flip == 1, negated, within) + jnp.where(upper, 64, 0)
    sign = jnp.where((flip == 1) & upper, -1.0, 1.0)
    select = jnp.where(col == target, sign, 0.0).astype(BF16)

    def turned(a):
        his, lows = [], []
        for j in range(GROUP):
            slot = jnp.where(flip == 1, GROUP - 1 - j, j)
            hi, low = split(d_ref[0, a, :, slot].reshape(HALF, 128))
            his.append(lax.dot_general(select, hi, NT, preferred_element_type=F32).astype(BF16))
            lows.append(lax.dot_general(select, low, NT, preferred_element_type=F32).astype(BF16))
        hi, low = jnp.concatenate(his, axis=0), jnp.concatenate(lows, axis=0)
        return mm(hi, wx_ref[0, a]) + mm(low, wx_ref[0, a]) + mm(hi, wx_ref[1, a])

    even, odd = turned(0), turned(1)
    for j in range(GROUP):

        def parts(v):
            re, im = v[128 * j : 128 * j + 64], v[128 * j + 64 : 128 * j + 128]
            return re[:, :HALF] + im[:, HALF:], im[:, :HALF] - re[:, HALF:]

        er, ei = parts(even)
        orr, oi = parts(odd)
        re = jnp.concatenate([er + orr, er - orr], axis=1)
        im = jnp.concatenate([ei + oi, ei - oi], axis=1)
        out_ref[0, j, 0] = re
        out_ref[1, j, 0] = im
        ky = 16 * px + 2 * (GROUP * step + j) + e
        my = (ky - jnp.where(ky >= HALF, N, 0)).astype(F32) * (1.0 / (cell_nm * N))
        mody = mod_smem[1, ky]
        msq = xz2[...] + my * my
        anchor = msq == 0.0
        inverse = 1.0 / jnp.where(anchor, 1.0, msq)
        decay = (math.pi**2 / beta_nm**2) * msq
        theta = jnp.where(anchor, 0.0, jnp.exp(-decay) * inverse * modxz[...] * mody)
        power = theta * (re * re + im * im)
        weight = power * (1.0 + decay) * inverse

        def rows(v):
            return jnp.sum(v.reshape(8, 8, N), axis=0)

        wz = weight * mz
        w0, w1, w2 = rows(weight), rows(wz), rows(wz * mz)
        acc[0] += rows(power)
        acc[1] += w0
        acc[2] += w0 * (my * my)
        acc[3] += w2
        acc[4] += w0 * my
        acc[5] += w1
        acc[6] += w1 * my

    @pl.when((e == 1) & (step == pl.num_programs(1) - 1))
    def _():
        def lanes(v):
            v = jnp.sum(v, axis=0, keepdims=True)
            return v[:, 0:128] + v[:, 128:256] + v[:, 256:384] + v[:, 384:512]

        sums_ref[...] = jnp.concatenate(
            [
                lanes(acc[0]),
                lanes(acc[1] * (mx * mx)),
                lanes(acc[2]),
                lanes(acc[3]),
                lanes(acc[4] * mx),
                lanes(acc[5] * mx),
                lanes(acc[6]),
                jnp.zeros((1, 128), F32),
            ],
            axis=0,
        )


def finish(gathered, place, moduli):
    wx = jnp.asarray(x_table())
    steps = 8 // GROUP

    def whole(shape):
        return pl.BlockSpec(shape, lambda e, s, flag: (0,) * len(shape))

    return pl.pallas_call(
        finish_kernel,
        out_shape=(
            jax.ShapeDtypeStruct((2, 8, 2, 64, N), F32),
            jax.ShapeDtypeStruct((8, 128), F32),
        ),
        grid_spec=pltpu.PrefetchScalarGridSpec(
            num_scalar_prefetch=1,
            grid=(2, steps),
            in_specs=[
                pl.BlockSpec(memory_space=pltpu.SMEM),
                pl.BlockSpec(
                    (1, 2, 32, GROUP, 8, 128),
                    lambda e, s, flag: (e, 0, 0, s + flag[0] * (steps - 1 - 2 * s), 0, 0),
                ),
                whole((2, 2, HALF, N)),
                whole((3, N)),
            ],
            out_specs=[
                pl.BlockSpec((2, GROUP, 1, 64, N), lambda e, s, flag: (0, s, e, 0, 0)),
                whole((8, 128)),
            ],
            scratch_shapes=[
                pltpu.VMEM((7, 8, N), F32),
                pltpu.VMEM((64, N), F32),
                pltpu.VMEM((64, N), F32),
            ],
        ),
        compiler_params=pltpu.CompilerParams(vmem_limit_bytes=62 * 2**20),
        name="finish",
    )(place, moduli, gathered, wx, moduli)


def total_kernel(part_ref, out_ref, first, second, middle, send, recv):
    yc, zh, c, lo, xc = [lax.axis_index(a) for a in AXES]
    inner = c * 8 + lo * 4 + xc
    outer = yc * 4 + zh

    def device(stage, t):
        if stage == 0:
            d = lax.rem(inner + t, 16)
            return yc, zh, lax.div(d, 8), lax.rem(lax.div(d, 4), 2), lax.rem(d, 4)
        d = lax.rem(outer + t, 16)
        return lax.div(d, 4), lax.rem(d, 4), c, lo, xc

    barrier = pltpu.get_barrier_semaphore()
    for stage in range(2):

        def greet(t, carry):
            pl.semaphore_signal(
                barrier, inc=1, device_id=device(stage, t), device_id_type=MESH
            )
            return carry

        lax.fori_loop(1, 16, greet, 0)
    pl.semaphore_wait(barrier, 30)

    def exchange_all(stage, source, slots, me):
        slots[me] = source[...]

        def put(t, carry):
            pltpu.make_async_remote_copy(
                src_ref=source,
                dst_ref=slots.at[me],
                send_sem=send.at[stage],
                recv_sem=recv.at[stage],
                device_id=device(stage, t),
                device_id_type=MESH,
            ).start()
            return carry

        lax.fori_loop(1, 16, put, 0)
        many = slots.at[pl.ds(0, 15)]
        pltpu.make_async_copy(many, many, recv.at[stage]).wait()
        return jnp.sum(slots[...], axis=0)

    middle[...] = exchange_all(0, part_ref, first, inner)
    out_ref[...] = jnp.broadcast_to(
        jnp.sum(exchange_all(1, middle, second, outer), axis=1, keepdims=True), (8, 128)
    )
    for stage in range(2):
        many = first.at[pl.ds(0, 15)]
        pltpu.make_async_copy(many, many, send.at[stage]).wait()


def total(parts):
    return pl.pallas_call(
        total_kernel,
        out_shape=jax.ShapeDtypeStruct((8, 128), F32),
        in_specs=[pl.BlockSpec(memory_space=pltpu.VMEM)],
        out_specs=pl.BlockSpec(memory_space=pltpu.VMEM),
        scratch_shapes=[
            pltpu.VMEM((16, 8, 128), F32),
            pltpu.VMEM((16, 8, 128), F32),
            pltpu.VMEM((8, 128), F32),
            pltpu.SemaphoreType.DMA((2,)),
            pltpu.SemaphoreType.DMA((2,)),
        ],
        compiler_params=pltpu.CompilerParams(collective_id=1, has_side_effects=True),
        name="total",
    )(parts)


def body(charges_old, spline_moduli):
    place = jnp.stack([lax.axis_index("py_0"), lax.axis_index(PX), lax.axis_index(PY)])
    gathered = exchange(charges_old).reshape(2, 2, 32, 8, 8, 128)
    structure, sums = finish(gathered, place.astype(jnp.int32), spline_moduli)
    totals = total(sums)[:, 0]
    energy = 0.5 * totals[0]
    virial = energy * jnp.array([1.0, 1.0, 1.0, 0.0, 0.0, 0.0], dtype=F32) - totals[1:7]
    return structure.reshape(2, 16, 64, N), energy, virial


def solution(mesh):
    torus = Mesh(mesh.devices.reshape(4, 4, 2, 2, 4), AXES)
    return jax.shard_map(
        body,
        mesh=torus,
        in_specs=(P(PX, PY, None, None, None), P()),
        out_specs=(P(None, PX, PY, None), P(), P()),
        check_vma=False,
    )
```

```python
import math

import jax
import jax.numpy as jnp
import numpy as np
from jax import lax
from jax.experimental import pallas as pl
from jax.experimental.pallas import tpu as pltpu
from jax.sharding import Mesh
from jax.sharding import PartitionSpec as P

AXES = ("px_0", "px_1", "px_2", "py_0", "py_1")
PX = AXES[:3]
PY = AXES[3:]
MESH = pl.DeviceIdType.MESH
F32 = jnp.float32
BF16 = jnp.bfloat16

beta_nm = 3.12
cell_nm = 0.1
N = 512
HALF = N // 2
NT = (((1,), (1,)), ((), ()))


def split_np(a):
    hi = a.astype(BF16)
    lo = (a - hi.astype(np.float64)).astype(BF16)
    return np.stack([hi, lo])


def angles(rows, cols):
    return 2.0 * math.pi * (np.outer(rows, cols) % N) / N


def z_table():
    z = np.arange(N)
    parts = []
    for b in range(4):
        t = angles(z, 64 * b + np.arange(64))
        parts += [np.cos(t), -np.sin(t)]
    edge = np.zeros((N, 128))
    for b in range(4):
        t = angles(z, np.array([64 * (b + 1)]))[:, 0]
        edge[:, 8 * b] = np.cos(t)
        edge[:, 64 + 8 * b] = -np.sin(t)
    return split_np(np.concatenate(parts + [edge], axis=1))


def half_table():
    r = np.arange(HALF)
    out = []
    for e in range(2):
        t = angles(2 * r + e, r)
        out.append(np.concatenate([np.cos(t), np.sin(t)], axis=1))
    return split_np(np.stack(out))


def split(v):
    hi = v.astype(BF16)
    return hi, (v - hi.astype(F32)).astype(BF16)


def mm(a, b):
    return jnp.dot(a, b, preferred_element_type=F32)


def signed_wave(mode_index):
    shifted = mode_index - N * (mode_index >= HALF).astype(jnp.int32)
    return shifted.astype(F32) / (cell_nm * N)


def ewald_kernel(
    mod_smem, mod_ref, x_hbm, wz_hbm, wh_hbm, out_hbm, energy_ref, virial_ref,
    x_ref, wz_ref, wh_ref, zs, r1, zy, r2, out_ref, acc, xz2, modxz, parts, first, middle, second,
    load, send1, recv1, send2, recv2, send3, recv3, leave,
):
    tables = ((x_hbm, x_ref), (wz_hbm, wz_ref), (wh_hbm, wh_ref))
    loads = [pltpu.make_async_copy(a, b, load.at[i]) for i, (a, b) in enumerate(tables)]
    for copy in loads:
        copy.start()

    yc, zh, c, lo, xc = [lax.axis_index(a) for a in AXES]
    p = yc * 8 + zh * 2 + c
    me16 = c * 8 + lo * 4 + xc
    me64 = p * 2 + lo
    outer = yc * 4 + zh
    b = xc + lo * (3 - 2 * xc)

    def peer16(t):
        d = lax.rem(me16 + t, 16)
        dc = lax.div(d, 8)
        dl = lax.rem(lax.div(d, 4), 2)
        dx = lax.rem(d, 4)
        return dc, dl, dx

    def peer64(t):
        d = lax.rem(me64 + t, 64)
        dp = lax.div(d, 2)
        dl = lax.rem(d, 2)
        dx = b + dl * (3 - 2 * b)
        return dp, dl, (lax.div(dp, 8), lax.rem(lax.div(dp, 2), 4), lax.rem(dp, 2), dl, dx)

    barrier = pltpu.get_barrier_semaphore()

    def greet16(t, carry):
        dc, dl, dx = peer16(t)
        pl.semaphore_signal(barrier, inc=1, device_id=(yc, zh, dc, dl, dx), device_id_type=MESH)
        return carry

    def greet64(t, carry):
        pl.semaphore_signal(barrier, inc=1, device_id=peer64(t)[2], device_id_type=MESH)
        return carry

    lax.fori_loop(1, 16, greet16, 0)
    lax.fori_loop(1, 64, greet64, 0)

    def z_step(g, carry):
        rows = x_ref[lax.div(g, 2), :, lax.rem(g, 2)].reshape(256, N)
        hi, low = split(rows)
        out = mm(hi, wz_ref[0]) + mm(low, wz_ref[0]) + mm(hi, wz_ref[1])
        for k in range(4):
            zs[g, k, 1:9] = out[:, 128 * k : 128 * k + 128].reshape(8, 32, 128)
        edge = out[:, 512:640].reshape(8, 32, 128)
        packed = edge[0]
        for r in range(1, 8):
            packed = packed + pltpu.roll(edge[r], r, 1)
        zs[g, 0, 0] = packed
        for k in range(1, 4):
            zs[g, k, 0] = pltpu.roll(packed, 128 - 8 * k, 1)
        return carry

    loads[0].wait()
    loads[1].wait()
    lax.fori_loop(0, 4, z_step, 0)
    pl.semaphore_wait(barrier, 78)

    my_rows = pl.ds(pl.multiple_of(me16 * 32, 32), 32)
    halves = (pl.ds(0, 5), pl.ds(5, 4))
    for h in range(2):

        def send_y(t, carry):
            dc, dl, dx = peer16(t)
            pltpu.make_async_remote_copy(
                src_ref=zs.at[2 * dc + dl, dx + dl * (3 - 2 * dx), halves[h]],
                dst_ref=r1.at[halves[h], my_rows, :],
                send_sem=send1.at[h],
                recv_sem=recv1.at[h],
                device_id=(yc, zh, dc, dl, dx),
                device_id_type=MESH,
            ).start()
            return carry

        lax.fori_loop(1, 16, send_y, 0)
    r1[:, my_rows, :] = zs[2 * c + lo, b]

    mx = signed_wave(lax.broadcasted_iota(jnp.int32, (1, N), 1))
    mz = signed_wave(64 * (4 * lo + xc) + lax.broadcasted_iota(jnp.int32, (64, 1), 0))
    acc[...] = jnp.zeros_like(acc)
    xz2[...] = mx * mx + mz * mz
    modz = pltpu.roll(jnp.broadcast_to(mod_ref[2:3, :], (8, N)), lax.rem(N - 64 * (4 * lo + xc), N), 1)
    modz = jnp.broadcast_to(modz[0:1, :128], (128, 128)).T[:64]
    modz = jnp.concatenate([modz] * 4, axis=1)
    modxz[...] = mod_ref[0:1, :] * modz * (1.0 / (math.pi * (cell_nm * N) ** 3))

    loads[2].wait()

    lane = lax.broadcasted_iota(jnp.int32, (HALF, 128), 1)
    is_edge = (lane == 0) | (lane == 64)
    turn = jnp.where(lane < 64, 1.0, -1.0).astype(F32)

    for h in range(2):
        many = r1.at[halves[h], pl.ds(0, 480), :]
        pltpu.make_async_copy(many, many, recv1.at[h]).wait()
        for e in range(2):
            base = MIRROR + 4 * (1 - e)

            def fold(i):
                top = r1[i, pl.ds(0, HALF), :]
                bottom = r1[i, pl.ds(HALF, HALF), :]
                return top + bottom if e == 0 else top - bottom

            for r in range(4):
                direct = fold(1 + 4 * h + r)
                edge = fold(0)
                if h or r:
                    edge = pltpu.roll(edge, 128 - (4 * h + r), 1)
                mirror = jnp.where(is_edge, edge, direct)
                plain = jnp.concatenate([direct, mirror], axis=1)
                turned = jnp.concatenate(
                    [pltpu.roll(direct, 64, 1) * turn, pltpu.roll(mirror, 64, 1) * turn], axis=1
                )
                hi, low = split(jnp.concatenate([plain, turned], axis=0))
                out = mm(wh_ref[0, e], hi) + mm(wh_ref[1, e], hi) + mm(wh_ref[0, e], low)
                zy[e, h, pl.ds(r, HALF, stride=4), :] = out[:, :128]
                zy[e, h, pl.ds(base + r, HALF, stride=4), :] = out[:, 128:]
                if e == 0:
                    zy[e, h, pl.ds(base + 4 * HALF + r, 1), :] = out[0:1, 128:]

            def rows_for(dp, dl):
                start = (1 - dl) * (32 * dp) + dl * (base + 4 * (249 - e) - 32 * dp)
                return zy.at[e, h, pl.ds(pl.multiple_of(start, 8), 32), :]

            own = (1 - lo) * (32 * p) + lo * (base + 4 * (249 - e) - 32 * p)
            r2[e, h, lo, p] = zy[e, h, pl.ds(pl.multiple_of(own, 8), 32), :]

            def send_x(t, carry):
                dp, dl, device = peer64(t)
                pltpu.make_async_remote_copy(
                    src_ref=rows_for(dp, dl),
                    dst_ref=r2.at[e, h, lo, p],
                    send_sem=send2.at[e, h],
                    recv_sem=recv2.at[e, h],
                    device_id=device,
                    device_id_type=MESH,
                ).start()
                return carry

            lax.fori_loop(1, 64, send_x, 0)

    flip = lo
    row = lax.broadcasted_iota(jnp.int32, (128, 128), 0)
    col = lax.broadcasted_iota(jnp.int32, (128, 128), 1)
    upper = row >= 64
    within = jnp.where(upper, row - 64, row)
    negated = jnp.where(within == 0, 0, 64 - within)
    target = jnp.where(flip == 1, negated, within) + jnp.where(upper, 64, 0)
    sign = jnp.where((flip == 1) & upper, -1.0, 1.0)
    select = jnp.where(col == target, sign, 0.0).astype(BF16)
    low_rows = lax.broadcasted_iota(jnp.int32, (32, 8, 128), 1) < 4

    def rows(v):
        return jnp.sum(v.reshape(8, 8, N), axis=0)

    for e in range(2):
        for h in range(2):
            many = zy.at[e, h, pl.ds(0, 63 * 32), :]
            pltpu.make_async_copy(many, many, recv2.at[e, h]).wait()

        def x_step(t, carry):
            tile = t + flip * (3 - 2 * t)

            def turned(a):
                top = r2[e, 0, a, :, pl.ds(pl.multiple_of(8 * tile, 8), 8), :]
                bottom = r2[e, 1, a, :, pl.ds(pl.multiple_of(8 * tile, 8), 8), :]
                slot0 = jnp.where(low_rows, top, pltpu.roll(bottom, 4, 1))
                slot1 = jnp.where(low_rows, pltpu.roll(top, 4, 1), bottom)
                his, lows = [], []
                for v in (jnp.where(flip == 1, slot1, slot0), jnp.where(flip == 1, slot0, slot1)):
                    hi, low = split(v.reshape(HALF, 128))
                    his.append(lax.dot_general(select, hi, NT, preferred_element_type=F32).astype(BF16))
                    lows.append(lax.dot_general(select, low, NT, preferred_element_type=F32).astype(BF16))
                hi, low = jnp.concatenate(his, axis=0), jnp.concatenate(lows, axis=0)
                return mm(hi, wh_ref[0, a]) + mm(low, wh_ref[0, a]) + mm(hi, wh_ref[1, a])

            even, odd = turned(0), turned(1)
            for j in range(2):

                def halves_of(v):
                    re, im = v[128 * j : 128 * j + 64], v[128 * j + 64 : 128 * j + 128]
                    return re[:, :HALF] + im[:, HALF:], im[:, :HALF] - re[:, HALF:]

                er, ei = halves_of(even)
                orr, oi = halves_of(odd)
                re = jnp.concatenate([er + orr, er - orr], axis=1)
                im = jnp.concatenate([ei + oi, ei - oi], axis=1)
                out_ref[0, 2 * t + j, e] = re
                out_ref[1, 2 * t + j, e] = im
                ky = 16 * p + 2 * (2 * t + j) + e
                my = (ky - jnp.where(ky >= HALF, N, 0)).astype(F32) * (1.0 / (cell_nm * N))
                mody = mod_smem[1, ky]
                msq = xz2[...] + my * my
                anchor = msq == 0.0
                inverse = 1.0 / jnp.where(anchor, 1.0, msq)
                decay = (math.pi**2 / beta_nm**2) * msq
                theta = jnp.where(anchor, 0.0, jnp.exp(-decay) * inverse * modxz[...] * mody)
                power = theta * (re * re + im * im)
                weight = power * (1.0 + decay) * inverse
                wz = weight * mz
                w0, w1, w2 = rows(weight), rows(wz), rows(wz * mz)
                acc[0] += rows(power)
                acc[1] += w0
                acc[2] += w0 * (my * my)
                acc[3] += w2
                acc[4] += w0 * my
                acc[5] += w1
                acc[6] += w1 * my
            block = pl.ds(2 * t, 2)
            pltpu.make_async_copy(out_ref.at[:, block, e], out_hbm.at[:, block, e], leave).start()
            return carry

        lax.fori_loop(0, 4, x_step, 0)

    def lanes(v):
        v = jnp.sum(v, axis=0, keepdims=True)
        return v[:, 0:128] + v[:, 128:256] + v[:, 256:384] + v[:, 384:512]

    parts[...] = jnp.concatenate(
        [
            lanes(acc[0]),
            lanes(acc[1] * (mx * mx)),
            lanes(acc[2]),
            lanes(acc[3]),
            lanes(acc[4] * mx),
            lanes(acc[5] * mx),
            lanes(acc[6]),
            jnp.zeros((1, 128), F32),
        ],
        axis=0,
    )

    def spread(stage, source, slots, me):
        slots[me] = source[...]

        def put(t, carry):
            if stage == 0:
                dc, dl, dx = peer16(t)
                device = (yc, zh, dc, dl, dx)
            else:
                d = lax.rem(outer + t, 16)
                device = (lax.div(d, 4), lax.rem(d, 4), c, lo, xc)
            pltpu.make_async_remote_copy(
                src_ref=source,
                dst_ref=slots.at[me],
                send_sem=send3.at[stage],
                recv_sem=recv3.at[stage],
                device_id=device,
                device_id_type=MESH,
            ).start()
            return carry

        lax.fori_loop(1, 16, put, 0)
        many = slots.at[pl.ds(0, 15)]
        pltpu.make_async_copy(many, many, recv3.at[stage]).wait()
        return jnp.sum(slots[...], axis=0)

    middle[...] = spread(0, parts, first, me16)
    totals = jnp.sum(spread(1, middle, second, outer), axis=1, keepdims=True)
    energy = 0.5 * totals[0:1]
    energy_ref[...] = jnp.broadcast_to(energy, (1, 128))
    sub8 = lax.broadcasted_iota(jnp.int32, (8, 128), 0)
    lane8 = lax.broadcasted_iota(jnp.int32, (8, 128), 1)
    full = jnp.where((sub8 >= 1) & (sub8 <= 3), energy, 0.0) - totals
    virial_ref[...] = jnp.sum(jnp.where(lane8 == sub8 - 1, full, 0.0), axis=0, keepdims=True)

    pltpu.make_async_copy(out_ref, out_hbm, leave).wait()
    for h in range(2):
        many = r1.at[halves[h], pl.ds(0, 480), :]
        pltpu.make_async_copy(many, many, send1.at[h]).wait()
        for e in range(2):
            sent = zy.at[e, h, pl.ds(0, 63 * 32), :]
            pltpu.make_async_copy(sent, sent, send2.at[e, h]).wait()
    for stage in range(2):
        many = first.at[pl.ds(0, 15)]
        pltpu.make_async_copy(many, many, send3.at[stage]).wait()


MIRROR = 1024
ROWS = 2064


def body(charges_old, spline_moduli):
    vmem, hbm = pl.BlockSpec(memory_space=pltpu.VMEM), pl.BlockSpec(memory_space=pl.ANY)
    dma = pltpu.SemaphoreType.DMA
    structure, energy, virial = pl.pallas_call(
        ewald_kernel,
        out_shape=(
            jax.ShapeDtypeStruct((2, 8, 2, 64, N), F32),
            jax.ShapeDtypeStruct((1, 128), F32),
            jax.ShapeDtypeStruct((1, 128), F32),
        ),
        in_specs=[pl.BlockSpec(memory_space=pltpu.SMEM), vmem] + [hbm] * 3,
        out_specs=(hbm, vmem, vmem),
        scratch_shapes=[
            pltpu.VMEM((2, 8, 2, 32, N), F32),
            pltpu.VMEM((2, N, 640), BF16),
            pltpu.VMEM((2, 2, HALF, N), BF16),
            pltpu.VMEM((4, 4, 9, 32, 128), F32),
            pltpu.VMEM((9, N, 128), F32),
            pltpu.VMEM((2, 2, ROWS, 128), F32),
            pltpu.VMEM((2, 2, 2, 32, 32, 128), F32),
            pltpu.VMEM((2, 8, 2, 64, N), F32),
            pltpu.VMEM((7, 8, N), F32),
            pltpu.VMEM((64, N), F32),
            pltpu.VMEM((64, N), F32),
            pltpu.VMEM((8, 128), F32),
            pltpu.VMEM((16, 8, 128), F32),
            pltpu.VMEM((8, 128), F32),
            pltpu.VMEM((16, 8, 128), F32),
            dma((3,)),
            dma((2,)),
            dma((2,)),
            dma((2, 2)),
            dma((2, 2)),
            dma((2,)),
            dma((2,)),
            dma,
        ],
        compiler_params=pltpu.CompilerParams(
            collective_id=0, has_side_effects=True, vmem_limit_bytes=62 * 2**20
        ),
        name="ewald",
    )(
        spline_moduli,
        spline_moduli,
        charges_old.reshape(2, 8, 2, 32, N),
        jnp.asarray(z_table()),
        jnp.asarray(half_table()),
    )
    return structure.reshape(2, 16, 64, N), energy[0, 0], virial[0, :6]


def solution(mesh):
    torus = Mesh(mesh.devices.reshape(4, 4, 2, 2, 4), AXES)
    return jax.shard_map(
        body,
        mesh=torus,
        in_specs=(P(PX, PY, None, None, None), P()),
        out_specs=(P(None, PX, PY, None), P(), P()),
        check_vma=False,
    )
```

```python
import math

import jax
import jax.numpy as jnp
import numpy as np
from jax import lax
from jax.experimental import pallas as pl
from jax.experimental.pallas import tpu as pltpu
from jax.sharding import Mesh
from jax.sharding import PartitionSpec as P

AXES = ("px_0", "px_1", "px_2", "py_0", "py_1")
PX = AXES[:3]
PY = AXES[3:]
MESH = pl.DeviceIdType.MESH
F32 = jnp.float32
BF16 = jnp.bfloat16

beta_nm = 3.12
cell_nm = 0.1
N = 512
HALF = N // 2
NT = (((1,), (1,)), ((), ()))


def split_np(a):
    hi = a.astype(BF16)
    lo = (a - hi.astype(np.float64)).astype(BF16)
    return np.stack([hi, lo])


def angles(rows, cols):
    return 2.0 * math.pi * (np.outer(rows, cols) % N) / N


def z_table():
    z = np.arange(N)
    parts = []
    for b in range(4):
        t = angles(z, 64 * b + np.arange(64))
        parts += [np.cos(t), -np.sin(t)]
    edge = np.zeros((N, 128))
    for b in range(4):
        t = angles(z, np.array([64 * (b + 1)]))[:, 0]
        edge[:, 8 * b] = np.cos(t)
        edge[:, 64 + 8 * b] = -np.sin(t)
    return split_np(np.concatenate(parts + [edge], axis=1))


def half_table():
    r = np.arange(HALF)
    out = []
    for e in range(2):
        t = angles(2 * r + e, r)
        out.append(np.concatenate([np.cos(t), np.sin(t)], axis=1))
    return split_np(np.stack(out))


def split(v):
    hi = v.astype(BF16)
    return hi, (v - hi.astype(F32)).astype(BF16)


def mm(a, b):
    return jnp.dot(a, b, preferred_element_type=F32)


def signed_wave(mode_index):
    shifted = mode_index - N * (mode_index >= HALF).astype(jnp.int32)
    return shifted.astype(F32) / (cell_nm * N)


def ewald_kernel(
    mod_smem, mod_ref, x_hbm, wz_hbm, wh_hbm, out_hbm, energy_ref, virial_ref,
    x_ref, wz_ref, wh_ref, zs, r1, zy, r2, out_ref, acc, xz2, modxz, parts, first, middle, second,
    load, send1, recv1, send2, recv2, send3, recv3, leave,
):
    tables = ((x_hbm, x_ref), (wz_hbm, wz_ref), (wh_hbm, wh_ref))
    loads = [pltpu.make_async_copy(a, b, load.at[i]) for i, (a, b) in enumerate(tables)]
    for copy in loads:
        copy.start()

    yc, zh, c, lo, xc = [lax.axis_index(a) for a in AXES]
    p = yc * 8 + zh * 2 + c
    me16 = c * 8 + lo * 4 + xc
    me64 = p * 2 + lo
    outer = yc * 4 + zh
    b = xc + lo * (3 - 2 * xc)

    def peer16(t):
        d = lax.rem(me16 + t, 16)
        dc = lax.div(d, 8)
        dl = lax.rem(lax.div(d, 4), 2)
        dx = lax.rem(d, 4)
        return dc, dl, dx

    def peer64(t):
        d = lax.rem(me64 + t, 64)
        dp = lax.div(d, 2)
        dl = lax.rem(d, 2)
        dx = b + dl * (3 - 2 * b)
        return dp, dl, (lax.div(dp, 8), lax.rem(lax.div(dp, 2), 4), lax.rem(dp, 2), dl, dx)

    barrier = pltpu.get_barrier_semaphore()

    def greet16(t, carry):
        dc, dl, dx = peer16(t)
        pl.semaphore_signal(barrier, inc=1, device_id=(yc, zh, dc, dl, dx), device_id_type=MESH)
        return carry

    def greet64(t, carry):
        far = lax.rem(t + 24, 63) + 1
        pl.semaphore_signal(barrier, inc=1, device_id=peer64(far)[2], device_id_type=MESH)
        return carry

    lax.fori_loop(0, 63, greet64, 0)
    lax.fori_loop(1, 16, greet16, 0)

    narrow = lax.rem(lax.broadcasted_iota(jnp.int32, (32, 128), 1), 64) < 8

    def z_step(g, carry):
        rows = x_ref[lax.div(g, 2), :, lax.rem(g, 2)].reshape(256, N)
        hi, low = split(rows)
        out = mm(hi, wz_ref[0]) + mm(low, wz_ref[0]) + mm(hi, wz_ref[1])
        for k in range(4):
            zs[g, k, 8:264] = out[:, 128 * k : 128 * k + 128]
        edge = out[:, 512:640].reshape(8, 32, 128)
        packed = edge[0]
        for r in range(1, 8):
            packed = packed + pltpu.roll(edge[r], r, 1)
        for k in range(4):
            one = pltpu.roll(packed, 128 - 8 * k, 1) if k else packed
            one = jnp.where(narrow, one, 0.0).reshape(4, 8, 128)
            zs[g, k, 0:8] = (
                one[0]
                + pltpu.roll(one[1], 8, 1)
                + pltpu.roll(one[2], 16, 1)
                + pltpu.roll(one[3], 24, 1)
            )
        return carry

    loads[0].wait()
    loads[1].wait()
    lax.fori_loop(0, 4, z_step, 0)
    pl.semaphore_wait(barrier, 78)

    halves = (pl.ds(0, 136), pl.ds(136, 128))
    for h in range(2):

        def send_y(t, carry):
            dc, dl, dx = peer16(t)
            pltpu.make_async_remote_copy(
                src_ref=zs.at[2 * dc + dl, dx + dl * (3 - 2 * dx), halves[h]],
                dst_ref=r1.at[me16, halves[h]],
                send_sem=send1.at[h],
                recv_sem=recv1.at[h],
                device_id=(yc, zh, dc, dl, dx),
                device_id_type=MESH,
            ).start()
            return carry

        lax.fori_loop(1, 16, send_y, 0)
    r1[me16] = zs[2 * c + lo, b]

    mx = signed_wave(lax.broadcasted_iota(jnp.int32, (1, N), 1))
    mz = signed_wave(64 * (4 * lo + xc) + lax.broadcasted_iota(jnp.int32, (64, 1), 0))
    acc[...] = jnp.zeros_like(acc)
    xz2[...] = mx * mx + mz * mz
    modz = pltpu.roll(jnp.broadcast_to(mod_ref[2:3, :], (8, N)), lax.rem(N - 64 * (4 * lo + xc), N), 1)
    modz = jnp.broadcast_to(modz[0:1, :128], (128, 128)).T[:64]
    modz = jnp.concatenate([modz] * 4, axis=1)
    modxz[...] = mod_ref[0:1, :] * modz * (1.0 / (math.pi * (cell_nm * N) ** 3))

    loads[2].wait()

    lane = lax.broadcasted_iota(jnp.int32, (HALF, 128), 1)
    is_edge = (lane == 0) | (lane == 64)
    turn = jnp.where(lane < 64, 1.0, -1.0).astype(F32)

    for h in range(2):
        many = r1.at[pl.ds(0, 15), halves[h]]
        pltpu.make_async_copy(many, many, recv1.at[h]).wait()
        for e in range(2):
            base = MIRROR + 4 * (1 - e)

            def fold(first, count):
                top = r1[0:8, first : first + count]
                bottom = r1[8:16, first : first + count]
                return top + bottom if e == 0 else top - bottom

            edges = fold(0, 8)
            for r in range(4):
                i = 4 * h + r
                direct = fold(8 + 32 * i, 32).reshape(HALF, 128)
                edge = jnp.stack(
                    [pltpu.roll(edges, 128 - 8 * k - i, 2) if k + i else edges for k in range(4)],
                    axis=1,
                ).reshape(HALF, 128)
                mirror = jnp.where(is_edge, edge, direct)
                plain = jnp.concatenate([direct, mirror], axis=1)
                turned = jnp.concatenate(
                    [pltpu.roll(direct, 64, 1) * turn, pltpu.roll(mirror, 64, 1) * turn], axis=1
                )
                hi, low = split(jnp.concatenate([plain, turned], axis=0))
                out = mm(wh_ref[0, e], hi) + mm(wh_ref[1, e], hi) + mm(wh_ref[0, e], low)
                zy[e, h, pl.ds(r, HALF, stride=4), :] = out[:, :128]
                zy[e, h, pl.ds(base + r, HALF, stride=4), :] = out[:, 128:]
                if e == 0:
                    zy[e, h, pl.ds(base + 4 * HALF + r, 1), :] = out[0:1, 128:]

            def start_for(dp, dl):
                return (1 - dl) * (32 * dp) + dl * (base + 4 * (249 - e) - 32 * dp)

            r2[e, h, lo, p] = zy[e, h, pl.ds(pl.multiple_of(start_for(p, lo), 8), 32), :]
            pieces = 2 if e and h else 1
            size = 32 // pieces
            for piece in range(pieces):

                def send_x(t, carry):
                    dp, dl, device = peer64(t)
                    skip = size * (piece + dl * (pieces - 1 - 2 * piece))
                    start = start_for(dp, dl) + skip
                    pltpu.make_async_remote_copy(
                        src_ref=zy.at[e, h, pl.ds(pl.multiple_of(start, 8), size), :],
                        dst_ref=r2.at[e, h, lo, p, pl.ds(pl.multiple_of(skip, 8), size), :],
                        send_sem=send2.at[2 * h + e + piece],
                        recv_sem=recv2.at[2 * h + e + piece],
                        device_id=device,
                        device_id_type=MESH,
                    ).start()
                    return carry

                lax.fori_loop(1, 64, send_x, 0)

    flip = lo
    row = lax.broadcasted_iota(jnp.int32, (128, 128), 0)
    col = lax.broadcasted_iota(jnp.int32, (128, 128), 1)
    upper = row >= 64
    within = jnp.where(upper, row - 64, row)
    negated = jnp.where(within == 0, 0, 64 - within)
    target = jnp.where(flip == 1, negated, within) + jnp.where(upper, 64, 0)
    sign = jnp.where((flip == 1) & upper, -1.0, 1.0)
    select = jnp.where(col == target, sign, 0.0).astype(BF16)
    low_rows = lax.broadcasted_iota(jnp.int32, (32, 8, 128), 1) < 4

    def rows(v):
        return jnp.sum(v.reshape(8, 8, N), axis=0)

    for e in range(2):

        def arrived(block, size):
            many = zy.at[0, 0, pl.ds(0, 63 * size), :]
            pltpu.make_async_copy(many, many, recv2.at[block]).wait()

        arrived(e, 32)
        if e == 0:
            arrived(2, 32)

        def x_step(t, carry):
            tile = t + flip * (3 - 2 * t)

            def turned(a):
                top = r2[e, 0, a, :, pl.ds(pl.multiple_of(8 * tile, 8), 8), :]
                bottom = r2[e, 1, a, :, pl.ds(pl.multiple_of(8 * tile, 8), 8), :]
                slot0 = jnp.where(low_rows, top, pltpu.roll(bottom, 4, 1))
                slot1 = jnp.where(low_rows, pltpu.roll(top, 4, 1), bottom)
                his, lows = [], []
                for v in (jnp.where(flip == 1, slot1, slot0), jnp.where(flip == 1, slot0, slot1)):
                    hi, low = split(v.reshape(HALF, 128))
                    his.append(lax.dot_general(select, hi, NT, preferred_element_type=F32).astype(BF16))
                    lows.append(lax.dot_general(select, low, NT, preferred_element_type=F32).astype(BF16))
                hi, low = jnp.concatenate(his, axis=0), jnp.concatenate(lows, axis=0)
                return mm(hi, wh_ref[0, a]) + mm(low, wh_ref[0, a]) + mm(hi, wh_ref[1, a])

            even, odd = turned(0), turned(1)
            for j in range(2):

                def halves_of(v):
                    re, im = v[128 * j : 128 * j + 64], v[128 * j + 64 : 128 * j + 128]
                    return re[:, :HALF] + im[:, HALF:], im[:, :HALF] - re[:, HALF:]

                er, ei = halves_of(even)
                orr, oi = halves_of(odd)
                re = jnp.concatenate([er + orr, er - orr], axis=1)
                im = jnp.concatenate([ei + oi, ei - oi], axis=1)
                out_ref[0, 2 * t + j, e] = re
                out_ref[1, 2 * t + j, e] = im
                ky = 16 * p + 2 * (2 * t + j) + e
                my = (ky - jnp.where(ky >= HALF, N, 0)).astype(F32) * (1.0 / (cell_nm * N))
                mody = mod_smem[1, ky]
                msq = xz2[...] + my * my
                anchor = msq == 0.0
                inverse = 1.0 / jnp.where(anchor, 1.0, msq)
                decay = (math.pi**2 / beta_nm**2) * msq
                theta = jnp.where(anchor, 0.0, jnp.exp(-decay) * inverse * modxz[...] * mody)
                power = theta * (re * re + im * im)
                weight = power * (1.0 + decay) * inverse
                wz = weight * mz
                w0, w1, w2 = rows(weight), rows(wz), rows(wz * mz)
                acc[0] += rows(power)
                acc[1] += w0
                acc[2] += w0 * (my * my)
                acc[3] += w2
                acc[4] += w0 * my
                acc[5] += w1
                acc[6] += w1 * my
            block = pl.ds(2 * t, 2)
            pltpu.make_async_copy(out_ref.at[:, block, e], out_hbm.at[:, block, e], leave).start()
            return carry

        if e == 0:
            lax.fori_loop(0, 4, x_step, 0)
        else:
            for piece in range(2):
                arrived(3 + piece, 16)
                x_step(2 * piece, 0)
                x_step(2 * piece + 1, 0)

    def lanes(v):
        v = jnp.sum(v, axis=0, keepdims=True)
        return v[:, 0:128] + v[:, 128:256] + v[:, 256:384] + v[:, 384:512]

    parts[...] = jnp.concatenate(
        [
            lanes(acc[0]),
            lanes(acc[1] * (mx * mx)),
            lanes(acc[2]),
            lanes(acc[3]),
            lanes(acc[4] * mx),
            lanes(acc[5] * mx),
            lanes(acc[6]),
            jnp.zeros((1, 128), F32),
        ],
        axis=0,
    )

    def spread(stage, source, slots, me):
        slots[me] = source[...]

        def put(t, carry):
            if stage == 0:
                dc, dl, dx = peer16(t)
                device = (yc, zh, dc, dl, dx)
            else:
                d = lax.rem(outer + t, 16)
                device = (lax.div(d, 4), lax.rem(d, 4), c, lo, xc)
            pltpu.make_async_remote_copy(
                src_ref=source,
                dst_ref=slots.at[me],
                send_sem=send3.at[stage],
                recv_sem=recv3.at[stage],
                device_id=device,
                device_id_type=MESH,
            ).start()
            return carry

        lax.fori_loop(1, 16, put, 0)
        many = slots.at[pl.ds(0, 15)]
        pltpu.make_async_copy(many, many, recv3.at[stage]).wait()
        return jnp.sum(slots[...], axis=0)

    middle[...] = spread(0, parts, first, me16)
    totals = jnp.sum(spread(1, middle, second, outer), axis=1, keepdims=True)
    energy = 0.5 * totals[0:1]
    energy_ref[...] = energy
    sub8 = lax.broadcasted_iota(jnp.int32, (8, 128), 0)
    lane8 = lax.broadcasted_iota(jnp.int32, (8, 128), 1)
    full = jnp.where((sub8 >= 1) & (sub8 <= 3), energy, 0.0) - totals
    virial_ref[...] = jnp.sum(jnp.where(lane8 == sub8 - 1, full, 0.0), axis=0, keepdims=True)[:, :6]

    pltpu.make_async_copy(out_ref, out_hbm, leave).wait()
    for h in range(2):
        many = r1.at[pl.ds(0, 15), halves[h]]
        pltpu.make_async_copy(many, many, send1.at[h]).wait()
    for block, size in enumerate((32, 32, 32, 16, 16)):
        sent = zy.at[0, 0, pl.ds(0, 63 * size), :]
        pltpu.make_async_copy(sent, sent, send2.at[block]).wait()
    for stage in range(2):
        many = first.at[pl.ds(0, 15)]
        pltpu.make_async_copy(many, many, send3.at[stage]).wait()


def copy_kernel(source, target, buffer, read, write):
    reads = [
        pltpu.make_async_copy(source.at[i], buffer.at[i], read.at[i]) for i in range(PIECES)
    ]
    writes = [
        pltpu.make_async_copy(buffer.at[i], target.at[i], write.at[i]) for i in range(PIECES)
    ]
    for copy in reads:
        copy.start()
    for i in range(PIECES):
        reads[i].wait()
        writes[i].start()
    for copy in writes:
        copy.wait()


def copy_out(array):
    return pl.pallas_call(
        copy_kernel,
        out_shape=jax.ShapeDtypeStruct(array.shape, F32),
        in_specs=[pl.BlockSpec(memory_space=pl.ANY)],
        out_specs=pl.BlockSpec(memory_space=pl.ANY),
        scratch_shapes=[
            pltpu.VMEM(array.shape, F32),
            pltpu.SemaphoreType.DMA((PIECES,)),
            pltpu.SemaphoreType.DMA((PIECES,)),
        ],
        compiler_params=pltpu.CompilerParams(vmem_limit_bytes=62 * 2**20),
        name="copy_out",
    )(array)


PIECES = 16
MIRROR = 1024
ROWS = 2064


def body(charges_old, spline_moduli):
    vmem, hbm = pl.BlockSpec(memory_space=pltpu.VMEM), pl.BlockSpec(memory_space=pl.ANY)
    dma = pltpu.SemaphoreType.DMA
    structure, energy, virial = pl.pallas_call(
        ewald_kernel,
        out_shape=(
            jax.ShapeDtypeStruct((2, 8, 2, 64, N), F32),
            jax.ShapeDtypeStruct((1, 1), F32),
            jax.ShapeDtypeStruct((1, 6), F32),
        ),
        in_specs=[pl.BlockSpec(memory_space=pltpu.SMEM), vmem] + [hbm] * 3,
        out_specs=(hbm, vmem, vmem),
        scratch_shapes=[
            pltpu.VMEM((2, 8, 2, 32, N), F32),
            pltpu.VMEM((2, N, 640), BF16),
            pltpu.VMEM((2, 2, HALF, N), BF16),
            pltpu.VMEM((4, 4, 264, 128), F32),
            pltpu.VMEM((16, 264, 128), F32),
            pltpu.VMEM((2, 2, ROWS, 128), F32),
            pltpu.VMEM((2, 2, 2, 32, 32, 128), F32),
            pltpu.VMEM((2, 8, 2, 64, N), F32),
            pltpu.VMEM((7, 8, N), F32),
            pltpu.VMEM((64, N), F32),
            pltpu.VMEM((64, N), F32),
            pltpu.VMEM((8, 128), F32),
            pltpu.VMEM((16, 8, 128), F32),
            pltpu.VMEM((8, 128), F32),
            pltpu.VMEM((16, 8, 128), F32),
            dma((3,)),
            dma((2,)),
            dma((2,)),
            dma((5,)),
            dma((5,)),
            dma((2,)),
            dma((2,)),
            dma,
        ],
        compiler_params=pltpu.CompilerParams(
            collective_id=0, has_side_effects=True, vmem_limit_bytes=62 * 2**20
        ),
        name="ewald",
    )(
        spline_moduli,
        spline_moduli,
        charges_old.reshape(2, 8, 2, 32, N),
        jnp.asarray(z_table()),
        jnp.asarray(half_table()),
    )
    structure = copy_out(structure.reshape(PIECES, -1, N))
    return structure.reshape(2, 16, 64, N), energy[0, 0], virial[0]


def solution(mesh):
    torus = Mesh(mesh.devices.reshape(4, 4, 2, 2, 4), AXES)
    return jax.shard_map(
        body,
        mesh=torus,
        in_specs=(P(PX, PY, None, None, None), P()),
        out_specs=(P(None, PX, PY, None), P(), P()),
        check_vma=False,
    )
```

```python
import math

import jax
import jax.numpy as jnp
import numpy as np
from jax import lax
from jax.experimental import pallas as pl
from jax.experimental.pallas import tpu as pltpu
from jax.sharding import Mesh
from jax.sharding import PartitionSpec as P

AXES = ("px_0", "px_1", "px_2", "py_0", "py_1")
PX = AXES[:3]
PY = AXES[3:]
MESH = pl.DeviceIdType.MESH
F32 = jnp.float32
BF16 = jnp.bfloat16

beta_nm = 3.12
cell_nm = 0.1
N = 512
HALF = N // 2
NT = (((1,), (1,)), ((), ()))


def split_np(a):
    hi = a.astype(BF16)
    lo = (a - hi.astype(np.float64)).astype(BF16)
    return np.stack([hi, lo])


def angles(rows, cols):
    return 2.0 * math.pi * (np.outer(rows, cols) % N) / N


def z_table():
    z = np.arange(N)
    parts = []
    for b in range(4):
        t = angles(z, 64 * b + np.arange(64))
        parts += [np.cos(t), -np.sin(t)]
    edge = np.zeros((N, 128))
    for b in range(4):
        t = angles(z, np.array([64 * (b + 1)]))[:, 0]
        edge[:, 8 * b] = np.cos(t)
        edge[:, 64 + 8 * b] = -np.sin(t)
    return split_np(np.concatenate(parts + [edge], axis=1))


def half_table():
    r = np.arange(HALF)
    out = []
    for e in range(2):
        t = angles(2 * r + e, r)
        out.append(np.concatenate([np.cos(t), np.sin(t)], axis=1))
    return split_np(np.stack(out))


def split(v):
    hi = v.astype(BF16)
    return hi, (v - hi.astype(F32)).astype(BF16)


def mm(a, b):
    return jnp.dot(a, b, preferred_element_type=F32)


def signed_wave(mode_index):
    shifted = mode_index - N * (mode_index >= HALF).astype(jnp.int32)
    return shifted.astype(F32) / (cell_nm * N)


def ewald_kernel(
    mod_hbm, x_hbm, wz_hbm, wh_hbm, out_ref, energy_ref, virial_ref,
    mod_smem, mod_ref, x_ref, wz_ref, wh_ref, zs, r1, zy, r2, acc, xz2, modxz, parts, first, middle, second,
    load, send1, recv1, send2, recv2, send3, recv3,
):
    tables = (
        (x_hbm, x_ref), (wz_hbm, wz_ref), (wh_hbm, wh_ref), (mod_hbm, mod_ref), (mod_hbm, mod_smem)
    )
    loads = [pltpu.make_async_copy(a, b, load.at[i]) for i, (a, b) in enumerate(tables)]
    for copy in loads:
        copy.start()

    yc, zh, c, lo, xc = [lax.axis_index(a) for a in AXES]
    p = yc * 8 + zh * 2 + c
    me16 = c * 8 + lo * 4 + xc
    me64 = p * 2 + lo
    outer = yc * 4 + zh
    b = xc + lo * (3 - 2 * xc)

    def peer16(t):
        d = lax.rem(me16 + t, 16)
        dc = lax.div(d, 8)
        dl = lax.rem(lax.div(d, 4), 2)
        dx = lax.rem(d, 4)
        return dc, dl, dx

    def peer64(t):
        d = lax.rem(me64 + t, 64)
        dp = lax.div(d, 2)
        dl = lax.rem(d, 2)
        dx = b + dl * (3 - 2 * b)
        return dp, dl, (lax.div(dp, 8), lax.rem(lax.div(dp, 2), 4), lax.rem(dp, 2), dl, dx)

    barrier = pltpu.get_barrier_semaphore()

    def greet16(t, carry):
        dc, dl, dx = peer16(t)
        pl.semaphore_signal(barrier, inc=1, device_id=(yc, zh, dc, dl, dx), device_id_type=MESH)
        return carry

    def greet64(t, carry):
        far = lax.rem(t + 24, 63) + 1
        pl.semaphore_signal(barrier, inc=1, device_id=peer64(far)[2], device_id_type=MESH)
        return carry

    lax.fori_loop(0, 63, greet64, 0, unroll=7)
    lax.fori_loop(1, 16, greet16, 0, unroll=5)

    narrow = lax.rem(lax.broadcasted_iota(jnp.int32, (32, 128), 1), 64) < 8

    def z_step(g, carry):
        rows = x_ref[lax.div(g, 2), :, lax.rem(g, 2)].reshape(256, N)
        hi, low = split(rows)
        out = mm(hi, wz_ref[0]) + mm(low, wz_ref[0]) + mm(hi, wz_ref[1])
        for k in range(4):
            zs[g, k, 8:264] = out[:, 128 * k : 128 * k + 128]
        edge = out[:, 512:640].reshape(8, 32, 128)
        packed = edge[0]
        for r in range(1, 8):
            packed = packed + pltpu.roll(edge[r], r, 1)
        for k in range(4):
            one = pltpu.roll(packed, 128 - 8 * k, 1) if k else packed
            one = jnp.where(narrow, one, 0.0).reshape(4, 8, 128)
            zs[g, k, 0:8] = (
                one[0]
                + pltpu.roll(one[1], 8, 1)
                + pltpu.roll(one[2], 16, 1)
                + pltpu.roll(one[3], 24, 1)
            )
        return carry

    loads[0].wait()
    loads[1].wait()
    lax.fori_loop(0, 4, z_step, 0)
    pl.semaphore_wait(barrier, 78)

    halves = (pl.ds(0, 136), pl.ds(136, 128))
    for h in range(2):

        def send_y(t, carry):
            d = lax.rem(c * 4 + xc + t, 8)
            dc, dx = lax.div(d, 4), lax.rem(d, 4)
            stay = lax.div(t, 8)
            dl = lo * stay + (1 - lo) * (1 - stay)
            pltpu.make_async_remote_copy(
                src_ref=zs.at[2 * dc + dl, dx + dl * (3 - 2 * dx), halves[h]],
                dst_ref=r1.at[me16, halves[h]],
                send_sem=send1.at[h],
                recv_sem=recv1.at[h],
                device_id=(yc, zh, dc, dl, dx),
                device_id_type=MESH,
            ).start()
            return carry

        lax.fori_loop(0, 8, send_y, 0, unroll=8)
        lax.fori_loop(9, 16, send_y, 0, unroll=7)
    r1[me16] = zs[2 * c + lo, b]

    loads[3].wait()
    loads[4].wait()
    mx = signed_wave(lax.broadcasted_iota(jnp.int32, (1, N), 1))
    mz = signed_wave(64 * (4 * lo + xc) + lax.broadcasted_iota(jnp.int32, (64, 1), 0))
    acc[...] = jnp.zeros_like(acc)
    xz2[...] = mx * mx + mz * mz
    modz = pltpu.roll(jnp.broadcast_to(mod_ref[2:3, :], (8, N)), lax.rem(N - 64 * (4 * lo + xc), N), 1)
    modz = jnp.broadcast_to(modz[0:1, :128], (128, 128)).T[:64]
    modz = jnp.concatenate([modz] * 4, axis=1)
    modxz[...] = mod_ref[0:1, :] * modz * (1.0 / (math.pi * (cell_nm * N) ** 3))

    loads[2].wait()

    lane = lax.broadcasted_iota(jnp.int32, (HALF, 128), 1)
    is_edge = (lane == 0) | (lane == 64)
    turn = jnp.where(lane < 64, 1.0, -1.0).astype(F32)

    for h in range(2):
        many = r1.at[pl.ds(0, 15), halves[h]]
        pltpu.make_async_copy(many, many, recv1.at[h]).wait()
        for e in range(2):
            base = MIRROR + 4 * (1 - e)

            def fold(first, count):
                top = r1[0:8, first : first + count]
                bottom = r1[8:16, first : first + count]
                return top + bottom if e == 0 else top - bottom

            edges = fold(0, 8)
            for r in range(4):
                i = 4 * h + r
                direct = fold(8 + 32 * i, 32).reshape(HALF, 128)
                edge = jnp.stack(
                    [pltpu.roll(edges, 128 - 8 * k - i, 2) if k + i else edges for k in range(4)],
                    axis=1,
                ).reshape(HALF, 128)
                mirror = jnp.where(is_edge, edge, direct)
                plain = jnp.concatenate([direct, mirror], axis=1)
                turned = jnp.concatenate(
                    [pltpu.roll(direct, 64, 1) * turn, pltpu.roll(mirror, 64, 1) * turn], axis=1
                )
                hi, low = split(jnp.concatenate([plain, turned], axis=0))
                out = mm(wh_ref[0, e], hi) + mm(wh_ref[1, e], hi) + mm(wh_ref[0, e], low)
                zy[e, h, pl.ds(r, HALF, stride=4), :] = out[:, :128]
                zy[e, h, pl.ds(base + r, HALF, stride=4), :] = out[:, 128:]
                if e == 0:
                    zy[e, h, pl.ds(base + 4 * HALF + r, 1), :] = out[0:1, 128:]

            def start_for(dp, dl):
                return (1 - dl) * (32 * dp) + dl * (base + 4 * (249 - e) - 32 * dp)

            r2[e, h, lo, p] = zy[e, h, pl.ds(pl.multiple_of(start_for(p, lo), 8), 32), :]
            pieces = 2 if e and h else 1
            size = 32 // pieces
            for piece in range(pieces):

                def send_x(k, turn_y):
                    part = lax.div(k + 1, 2)
                    dz = lax.rem(2 * zh + lo + 4 + part * (1 - 2 * lax.rem(k, 2)), 8)
                    dzh, dl = lax.div(dz, 2), lax.rem(dz, 2)
                    dy = lax.rem(yc + turn_y // 2, 4)
                    dc = lax.rem(c + turn_y % 2, 2)
                    dp = dy * 8 + dzh * 2 + dc
                    device = (dy, dzh, dc, dl, b + dl * (3 - 2 * b))
                    skip = size * (piece + dl * (pieces - 1 - 2 * piece))
                    start = start_for(dp, dl) + skip
                    pltpu.make_async_remote_copy(
                        src_ref=zy.at[e, h, pl.ds(pl.multiple_of(start, 8), size), :],
                        dst_ref=r2.at[e, h, lo, p, pl.ds(pl.multiple_of(skip, 8), size), :],
                        send_sem=send2.at[2 * h + e + piece],
                        recv_sem=recv2.at[2 * h + e + piece],
                        device_id=device,
                        device_id_type=MESH,
                    ).start()

                def send_plane(k, carry):
                    for i in range(8):
                        send_x(k, i)
                    return carry

                lax.fori_loop(0, 7, send_plane, 0)
                for i in range(1, 8):
                    send_x(7, i)

    flip = lo
    row = lax.broadcasted_iota(jnp.int32, (128, 128), 0)
    col = lax.broadcasted_iota(jnp.int32, (128, 128), 1)
    upper = row >= 64
    within = jnp.where(upper, row - 64, row)
    negated = jnp.where(within == 0, 0, 64 - within)
    target = jnp.where(flip == 1, negated, within) + jnp.where(upper, 64, 0)
    sign = jnp.where((flip == 1) & upper, -1.0, 1.0)
    select = jnp.where(col == target, sign, 0.0).astype(BF16)
    low_rows = lax.broadcasted_iota(jnp.int32, (32, 8, 128), 1) < 4

    def rows(v):
        return jnp.sum(v.reshape(8, 8, N), axis=0)

    for e in range(2):

        def arrived(block, size):
            many = zy.at[0, 0, pl.ds(0, 63 * size), :]
            pltpu.make_async_copy(many, many, recv2.at[block]).wait()

        arrived(e, 32)
        if e == 0:
            arrived(2, 32)

        def x_step(t, carry):
            tile = t + flip * (3 - 2 * t)

            def turned(a):
                top = r2[e, 0, a, :, pl.ds(pl.multiple_of(8 * tile, 8), 8), :]
                bottom = r2[e, 1, a, :, pl.ds(pl.multiple_of(8 * tile, 8), 8), :]
                slot0 = jnp.where(low_rows, top, pltpu.roll(bottom, 4, 1))
                slot1 = jnp.where(low_rows, pltpu.roll(top, 4, 1), bottom)
                his, lows = [], []
                for v in (jnp.where(flip == 1, slot1, slot0), jnp.where(flip == 1, slot0, slot1)):
                    hi, low = split(v.reshape(HALF, 128))
                    his.append(lax.dot_general(select, hi, NT, preferred_element_type=F32).astype(BF16))
                    lows.append(lax.dot_general(select, low, NT, preferred_element_type=F32).astype(BF16))
                hi, low = jnp.concatenate(his, axis=0), jnp.concatenate(lows, axis=0)
                return mm(hi, wh_ref[0, a]) + mm(low, wh_ref[0, a]) + mm(hi, wh_ref[1, a])

            even, odd = turned(0), turned(1)
            for j in range(2):

                def halves_of(v):
                    re, im = v[128 * j : 128 * j + 64], v[128 * j + 64 : 128 * j + 128]
                    return re[:, :HALF] + im[:, HALF:], im[:, :HALF] - re[:, HALF:]

                er, ei = halves_of(even)
                orr, oi = halves_of(odd)
                re = jnp.concatenate([er + orr, er - orr], axis=1)
                im = jnp.concatenate([ei + oi, ei - oi], axis=1)
                out_ref[0, 2 * t + j, e] = re
                out_ref[1, 2 * t + j, e] = im
                ky = 16 * p + 2 * (2 * t + j) + e
                my = (ky - jnp.where(ky >= HALF, N, 0)).astype(F32) * (1.0 / (cell_nm * N))
                mody = mod_smem[1, ky]
                msq = xz2[...] + my * my
                anchor = msq == 0.0
                inverse = 1.0 / jnp.where(anchor, 1.0, msq)
                decay = (math.pi**2 / beta_nm**2) * msq
                theta = jnp.where(anchor, 0.0, jnp.exp(-decay) * inverse * modxz[...] * mody)
                power = theta * (re * re + im * im)
                weight = power * (1.0 + decay) * inverse
                wz = weight * mz
                w0, w1, w2 = rows(weight), rows(wz), rows(wz * mz)
                acc[0] += rows(power)
                acc[1] += w0
                acc[2] += w0 * (my * my)
                acc[3] += w2
                acc[4] += w0 * my
                acc[5] += w1
                acc[6] += w1 * my
            return carry

        if e == 0:
            lax.fori_loop(0, 4, x_step, 0)
        else:
            for piece in range(2):
                arrived(3 + piece, 16)
                x_step(2 * piece, 0)
                x_step(2 * piece + 1, 0)

    def lanes(v):
        v = jnp.sum(v, axis=0, keepdims=True)
        return v[:, 0:128] + v[:, 128:256] + v[:, 256:384] + v[:, 384:512]

    parts[...] = jnp.concatenate(
        [
            lanes(acc[0]),
            lanes(acc[1] * (mx * mx)),
            lanes(acc[2]),
            lanes(acc[3]),
            lanes(acc[4] * mx),
            lanes(acc[5] * mx),
            lanes(acc[6]),
            jnp.zeros((1, 128), F32),
        ],
        axis=0,
    )

    def spread(stage, source, slots, me):
        slots[me] = source[...]

        def put(t, carry):
            if stage == 0:
                dc, dl, dx = peer16(t)
                device = (yc, zh, dc, dl, dx)
            else:
                d = lax.rem(outer + t, 16)
                device = (lax.div(d, 4), lax.rem(d, 4), c, lo, xc)
            pltpu.make_async_remote_copy(
                src_ref=source,
                dst_ref=slots.at[me],
                send_sem=send3.at[stage],
                recv_sem=recv3.at[stage],
                device_id=device,
                device_id_type=MESH,
            ).start()
            return carry

        lax.fori_loop(1, 16, put, 0, unroll=5)
        many = slots.at[pl.ds(0, 15)]
        pltpu.make_async_copy(many, many, recv3.at[stage]).wait()
        return jnp.sum(slots[...], axis=0)

    middle[...] = spread(0, parts, first, me16)
    totals = jnp.sum(spread(1, middle, second, outer), axis=1, keepdims=True)
    energy = 0.5 * totals[0:1]
    energy_ref[...] = energy
    sub8 = lax.broadcasted_iota(jnp.int32, (8, 128), 0)
    lane8 = lax.broadcasted_iota(jnp.int32, (8, 128), 1)
    full = jnp.where((sub8 >= 1) & (sub8 <= 3), energy, 0.0) - totals
    virial_ref[...] = jnp.sum(jnp.where(lane8 == sub8 - 1, full, 0.0), axis=0, keepdims=True)[:, :6]

    for h in range(2):
        many = r1.at[pl.ds(0, 15), halves[h]]
        pltpu.make_async_copy(many, many, send1.at[h]).wait()
    for block, size in enumerate((32, 32, 32, 16, 16)):
        sent = zy.at[0, 0, pl.ds(0, 63 * size), :]
        pltpu.make_async_copy(sent, sent, send2.at[block]).wait()
    for stage in range(2):
        many = first.at[pl.ds(0, 15)]
        pltpu.make_async_copy(many, many, send3.at[stage]).wait()


MIRROR = 1024
ROWS = 2064


def body(charges_old, spline_moduli):
    vmem, hbm = pl.BlockSpec(memory_space=pltpu.VMEM), pl.BlockSpec(memory_space=pl.ANY)
    dma = pltpu.SemaphoreType.DMA
    structure, energy, virial = pl.pallas_call(
        ewald_kernel,
        out_shape=(
            jax.ShapeDtypeStruct((2, 8, 2, 64, N), F32),
            jax.ShapeDtypeStruct((1, 1), F32),
            jax.ShapeDtypeStruct((1, 6), F32),
        ),
        in_specs=[hbm] * 4,
        out_specs=(vmem, vmem, vmem),
        scratch_shapes=[
            pltpu.SMEM((3, N), F32),
            pltpu.VMEM((3, N), F32),
            pltpu.VMEM((2, 8, 2, 32, N), F32),
            pltpu.VMEM((2, N, 640), BF16),
            pltpu.VMEM((2, 2, HALF, N), BF16),
            pltpu.VMEM((4, 4, 264, 128), F32),
            pltpu.VMEM((16, 264, 128), F32),
            pltpu.VMEM((2, 2, ROWS, 128), F32),
            pltpu.VMEM((2, 2, 2, 32, 32, 128), F32),
            pltpu.VMEM((7, 8, N), F32),
            pltpu.VMEM((64, N), F32),
            pltpu.VMEM((64, N), F32),
            pltpu.VMEM((8, 128), F32),
            pltpu.VMEM((16, 8, 128), F32),
            pltpu.VMEM((8, 128), F32),
            pltpu.VMEM((16, 8, 128), F32),
            dma((5,)),
            dma((2,)),
            dma((2,)),
            dma((5,)),
            dma((5,)),
            dma((2,)),
            dma((2,)),
        ],
        compiler_params=pltpu.CompilerParams(
            collective_id=0, has_side_effects=True, vmem_limit_bytes=24 * 2**20
        ),
        name="ewald",
    )(
        *[
            pltpu.with_memory_space_constraint(operand, pltpu.HBM)
            for operand in (
                spline_moduli,
                charges_old.reshape(2, 8, 2, 32, N),
                jnp.asarray(z_table()),
                jnp.asarray(half_table()),
            )
        ]
    )
    return structure.reshape(2, 16, 64, N), energy[0, 0], virial[0]


def solution(mesh):
    torus = Mesh(mesh.devices.reshape(4, 4, 2, 2, 4), AXES)
    return jax.shard_map(
        body,
        mesh=torus,
        in_specs=(P(PX, PY, None, None, None), P()),
        out_specs=(P(None, PX, PY, None), P(), P()),
        check_vma=False,
    )
```

```python
import math

import jax
import jax.numpy as jnp
import numpy as np
from jax import lax
from jax.experimental import pallas as pl
from jax.experimental.pallas import tpu as pltpu
from jax.sharding import Mesh
from jax.sharding import PartitionSpec as P

AXES = ("px_0", "px_1", "px_2", "py_0", "py_1")
PX = AXES[:3]
PY = AXES[3:]
MESH = pl.DeviceIdType.MESH
F32 = jnp.float32
BF16 = jnp.bfloat16

beta_nm = 3.12
cell_nm = 0.1
N = 512
HALF = N // 2
NT = (((1,), (1,)), ((), ()))


def split_np(a):
    hi = a.astype(BF16)
    lo = (a - hi.astype(np.float64)).astype(BF16)
    return np.stack([hi, lo])


def angles(rows, cols):
    return 2.0 * math.pi * (np.outer(rows, cols) % N) / N


def z_table():
    z = np.arange(N)
    parts = []
    for b in range(4):
        t = angles(z, 64 * b + np.arange(64))
        parts += [np.cos(t), -np.sin(t)]
    edge = np.zeros((N, 128))
    for b in range(4):
        t = angles(z, np.array([64 * (b + 1)]))[:, 0]
        edge[:, 8 * b] = np.cos(t)
        edge[:, 64 + 8 * b] = -np.sin(t)
    return split_np(np.concatenate(parts + [edge], axis=1))


def half_table():
    r = np.arange(HALF)
    out = []
    for e in range(2):
        t = angles(2 * r + e, r)
        out.append(np.concatenate([np.cos(t), np.sin(t)], axis=1))
    return split_np(np.stack(out))


def split(v):
    hi = v.astype(BF16)
    return hi, (v - hi.astype(F32)).astype(BF16)


def mm(a, b):
    return jnp.dot(a, b, preferred_element_type=F32)


def signed_wave(mode_index):
    shifted = mode_index - N * (mode_index >= HALF).astype(jnp.int32)
    return shifted.astype(F32) / (cell_nm * N)


def ewald_kernel(
    mod_hbm, x_hbm, wz_hbm, wh_hbm, out_ref, energy_ref, virial_ref,
    mod_smem, mod_ref, x_ref, wz_ref, wh_ref, wy_ref, zs, r1, zy, r2, acc, xz2, modxz, parts, first, middle, second,
    load, send1, recv1, send2, recv2, send3, recv3,
):
    tables = (
        (x_hbm, x_ref), (wz_hbm, wz_ref), (wh_hbm, wh_ref), (mod_hbm, mod_ref), (mod_hbm, mod_smem)
    )
    loads = [pltpu.make_async_copy(a, b, load.at[i]) for i, (a, b) in enumerate(tables)]
    for copy in loads:
        copy.start()

    yc, zh, c, lo, xc = [lax.axis_index(a) for a in AXES]
    p = yc * 8 + zh * 2 + c
    me16 = c * 8 + lo * 4 + xc
    me64 = p * 2 + lo
    outer = yc * 4 + zh
    b = xc + lo * (3 - 2 * xc)

    def peer16(t):
        d = lax.rem(me16 + t, 16)
        dc = lax.div(d, 8)
        dl = lax.rem(lax.div(d, 4), 2)
        dx = lax.rem(d, 4)
        return dc, dl, dx

    def peer64(t):
        d = lax.rem(me64 + t, 64)
        dp = lax.div(d, 2)
        dl = lax.rem(d, 2)
        dx = b + dl * (3 - 2 * b)
        return dp, dl, (lax.div(dp, 8), lax.rem(lax.div(dp, 2), 4), lax.rem(dp, 2), dl, dx)

    barrier = pltpu.get_barrier_semaphore()

    def greet16(t, carry):
        dc, dl, dx = peer16(t)
        pl.semaphore_signal(barrier, inc=1, device_id=(yc, zh, dc, dl, dx), device_id_type=MESH)
        return carry

    def greet64(t, carry):
        far = lax.rem(t + 24, 63) + 1
        pl.semaphore_signal(barrier, inc=1, device_id=peer64(far)[2], device_id_type=MESH)
        return carry

    lax.fori_loop(0, 63, greet64, 0, unroll=7)
    lax.fori_loop(1, 16, greet16, 0, unroll=5)

    narrow = lax.rem(lax.broadcasted_iota(jnp.int32, (32, 128), 1), 64) < 8

    def z_step(g, carry):
        rows = x_ref[lax.div(g, 2), :, lax.rem(g, 2)].reshape(256, N)
        hi, low = split(rows)
        out = mm(hi, wz_ref[0]) + mm(low, wz_ref[0]) + mm(hi, wz_ref[1])
        for k in range(4):
            zs[g, k, 8:264] = out[:, 128 * k : 128 * k + 128]
        edge = out[:, 512:640].reshape(8, 32, 128)
        packed = edge[0]
        for r in range(1, 8):
            packed = packed + pltpu.roll(edge[r], r, 1)
        for k in range(4):
            one = pltpu.roll(packed, 128 - 8 * k, 1) if k else packed
            one = jnp.where(narrow, one, 0.0).reshape(4, 8, 128)
            zs[g, k, 0:8] = (
                one[0]
                + pltpu.roll(one[1], 8, 1)
                + pltpu.roll(one[2], 16, 1)
                + pltpu.roll(one[3], 24, 1)
            )
        return carry

    loads[0].wait()
    loads[1].wait()
    lax.fori_loop(0, 4, z_step, 0)
    pl.semaphore_wait(barrier, 78)

    for h in range(2):

        def send_y(t, carry):
            d = lax.rem(c * 4 + xc + t, 8)
            dc, dx = lax.div(d, 4), lax.rem(d, 4)
            stay = lax.div(t, 8)
            dl = lo * stay + (1 - lo) * (1 - stay)
            pltpu.make_async_remote_copy(
                src_ref=zs.at[2 * dc + h, dx + dl * (3 - 2 * dx)],
                dst_ref=r1.at[h, me16],
                send_sem=send1.at[h],
                recv_sem=recv1.at[h],
                device_id=(yc, zh, dc, dl, dx),
                device_id_type=MESH,
            ).start()
            return carry

        lax.fori_loop(0, 8, send_y, 0, unroll=8)
        lax.fori_loop(9, 16, send_y, 0, unroll=7)
    for h in range(2):
        r1[h, me16] = zs[2 * c + h, b]

    loads[3].wait()
    loads[4].wait()
    mx = signed_wave(lax.broadcasted_iota(jnp.int32, (1, N), 1))
    mz = signed_wave(64 * (4 * lo + xc) + lax.broadcasted_iota(jnp.int32, (64, 1), 0))
    acc[...] = jnp.zeros_like(acc)
    xz2[...] = mx * mx + mz * mz
    modz = pltpu.roll(jnp.broadcast_to(mod_ref[2:3, :], (8, N)), lax.rem(N - 64 * (4 * lo + xc), N), 1)
    modz = jnp.broadcast_to(modz[0:1, :128], (128, 128)).T[:64]
    modz = jnp.concatenate([modz] * 4, axis=1)
    modxz[...] = mod_ref[0:1, :] * modz * (1.0 / (math.pi * (cell_nm * N) ** 3))

    loads[2].wait()

    def plane(d):
        dz = lax.rem(2 * zh + lo + 8 + d * (2 * lo - 1), 8)
        return lax.div(dz, 2), lax.rem(dz, 2)

    for kind in range(2):
        for near in range(2):
            zhp = plane(2 * near + lo + kind - 2 * lo * kind)[0]
            for e in range(2):
                for part in range(2):
                    for y in range(4):
                        start = pl.multiple_of(64 * y + 16 * zhp, 16)
                        wy_ref[e, part, pl.ds(128 * kind + 64 * near + 16 * y, 16), :] = wh_ref[
                            part, e, pl.ds(start, 16), :
                        ]

    lane = lax.broadcasted_iota(jnp.int32, (HALF, 128), 1)
    is_edge = (lane == 0) | (lane == 64)
    turn = jnp.where(lane < 64, 1.0, -1.0).astype(F32)

    for h in range(2):
        many = r1.at[0, pl.ds(0, 15)]
        pltpu.make_async_copy(many, many, recv1.at[h]).wait()
        for e in range(2):

            def fold(first, count):
                top = r1[h, 0:8, first : first + count]
                bottom = r1[h, 8:16, first : first + count]
                return top + bottom if e == 0 else top - bottom

            edges = fold(0, 8)
            for pair in range(4):
                tiles = [[], []]
                for r in (2 * pair, 2 * pair + 1):
                    direct = fold(8 + 32 * r, 32).reshape(HALF, 128)
                    edge = jnp.stack(
                        [pltpu.roll(edges, 128 - 8 * k - r, 2) if k + r else edges for k in range(4)],
                        axis=1,
                    ).reshape(HALF, 128)
                    tiles[0].append(direct)
                    tiles[1].append(jnp.where(is_edge, edge, direct) * turn)
                for kind in range(2):
                    plain = jnp.concatenate(tiles[kind], axis=1)
                    turned = jnp.concatenate([pltpu.roll(v, 64, 1) * turn for v in tiles[kind]], axis=1)
                    hi, low = split(jnp.concatenate([plain, turned], axis=0))
                    rows_of = pl.ds(128 * kind, 128)
                    high, small = wy_ref[e, 0, rows_of, :], wy_ref[e, 1, rows_of, :]
                    out = mm(high, hi) + mm(small, hi) + mm(high, low)
                    for k in range(2):
                        start = 1024 * kind + 2 * pair + k
                        zy[e, h, pl.ds(start, 128, stride=8), :] = out[:, 128 * k : 128 * k + 128]

            def start_for(kind, near, y, core):
                return pl.multiple_of(8 * (128 * kind + 64 * near + 16 * y + 8 * core), 64)

            r2[e, h, p] = zy[e, h, pl.ds(start_for(lo, 0, yc, c), 64), :]
            pieces = 2 if e and h else 1
            size = 64 // pieces
            for piece in range(pieces):

                def send_x(d, i):
                    zhp, dl = plane(d)
                    dy = lax.rem(yc + i // 2, 4)
                    dc = lax.rem(c + i % 2, 2)
                    start = start_for(dl, lax.div(d, 2), dy, dc) + size * piece
                    pltpu.make_async_remote_copy(
                        src_ref=zy.at[e, h, pl.ds(pl.multiple_of(start, 8), size), :],
                        dst_ref=r2.at[e, h, p, pl.ds(size * piece, size), :],
                        send_sem=send2.at[2 * h + e + piece],
                        recv_sem=recv2.at[2 * h + e + piece],
                        device_id=(dy, zhp, dc, dl, b + dl * (3 - 2 * b)),
                        device_id_type=MESH,
                    ).start()

                def send_plane(k, carry):
                    for i in range(8):
                        send_x(3 - k, i)
                    return carry

                lax.fori_loop(0, 3, send_plane, 0)
                for i in range(1, 8):
                    send_x(jnp.int32(0), i)

    flip = lo
    row = lax.broadcasted_iota(jnp.int32, (128, 128), 0)
    col = lax.broadcasted_iota(jnp.int32, (128, 128), 1)
    upper = row >= 64
    within = jnp.where(upper, row - 64, row)
    negated = jnp.where(within == 0, 0, 64 - within)
    target = jnp.where(flip == 1, negated, within) + jnp.where(upper, 64, 0)
    select = jnp.where(col == target, 1.0, 0.0).astype(BF16)

    def rows(v):
        return jnp.sum(v.reshape(8, 8, N), axis=0)

    for e in range(2):

        def arrived(block, size):
            many = zy.at[0, 0, pl.ds(0, 31 * size), :]
            pltpu.make_async_copy(many, many, recv2.at[block]).wait()

        arrived(e, 64)
        if e == 0:
            arrived(2, 64)

        def x_step(t, carry):
            def turned(a):
                his, lows = [], []
                for j in range(2):
                    v = r2[e, a, :, pl.ds(pl.multiple_of(8 * (2 * t + j), 8), 8), :]
                    hi, low = split(v.reshape(HALF, 128))
                    his.append(lax.dot_general(select, hi, NT, preferred_element_type=F32).astype(BF16))
                    lows.append(lax.dot_general(select, low, NT, preferred_element_type=F32).astype(BF16))
                hi, low = jnp.concatenate(his, axis=0), jnp.concatenate(lows, axis=0)
                return mm(hi, wh_ref[0, a]) + mm(low, wh_ref[0, a]) + mm(hi, wh_ref[1, a])

            even, odd = turned(0), turned(1)
            for j in range(2):

                def halves_of(v):
                    re, im = v[128 * j : 128 * j + 64], v[128 * j + 64 : 128 * j + 128]
                    return re[:, :HALF] + im[:, HALF:], im[:, :HALF] - re[:, HALF:]

                er, ei = halves_of(even)
                orr, oi = halves_of(odd)
                re = jnp.concatenate([er + orr, er - orr], axis=1)
                im = jnp.concatenate([ei + oi, ei - oi], axis=1)
                out_ref[0, 2 * t + j, e] = re
                out_ref[1, 2 * t + j, e] = im
                ky = 16 * p + 2 * (2 * t + j) + e
                my = (ky - jnp.where(ky >= HALF, N, 0)).astype(F32) * (1.0 / (cell_nm * N))
                mody = mod_smem[1, ky]
                msq = xz2[...] + my * my
                anchor = msq == 0.0
                inverse = 1.0 / jnp.where(anchor, 1.0, msq)
                decay = (math.pi**2 / beta_nm**2) * msq
                theta = jnp.where(anchor, 0.0, jnp.exp(-decay) * inverse * modxz[...] * mody)
                power = theta * (re * re + im * im)
                weight = power * (1.0 + decay) * inverse
                wz = weight * mz
                w0, w1, w2 = rows(weight), rows(wz), rows(wz * mz)
                acc[0] += rows(power)
                acc[1] += w0
                acc[2] += w0 * (my * my)
                acc[3] += w2
                acc[4] += w0 * my
                acc[5] += w1
                acc[6] += w1 * my
            return carry

        if e == 0:
            lax.fori_loop(0, 4, x_step, 0)
        else:
            for piece in range(2):
                arrived(3 + piece, 32)
                x_step(2 * piece, 0)
                x_step(2 * piece + 1, 0)

    def lanes(v):
        v = jnp.sum(v, axis=0, keepdims=True)
        return v[:, 0:128] + v[:, 128:256] + v[:, 256:384] + v[:, 384:512]

    parts[...] = jnp.concatenate(
        [
            lanes(acc[0]),
            lanes(acc[1] * (mx * mx)),
            lanes(acc[2]),
            lanes(acc[3]),
            lanes(acc[4] * mx),
            lanes(acc[5] * mx),
            lanes(acc[6]),
            jnp.zeros((1, 128), F32),
        ],
        axis=0,
    )

    def spread(stage, source, slots, me):
        slots[me] = source[...]

        def put(t, carry):
            if stage == 0:
                dc, dl, dx = peer16(t)
                device = (yc, zh, dc, dl, dx)
            else:
                d = lax.rem(outer + t, 16)
                device = (lax.div(d, 4), lax.rem(d, 4), c, lo, xc)
            pltpu.make_async_remote_copy(
                src_ref=source,
                dst_ref=slots.at[me],
                send_sem=send3.at[stage],
                recv_sem=recv3.at[stage],
                device_id=device,
                device_id_type=MESH,
            ).start()
            return carry

        lax.fori_loop(1, 16, put, 0, unroll=5)
        many = slots.at[pl.ds(0, 15)]
        pltpu.make_async_copy(many, many, recv3.at[stage]).wait()
        return jnp.sum(slots[...], axis=0)

    middle[...] = spread(0, parts, first, me16)
    totals = jnp.sum(spread(1, middle, second, outer), axis=1, keepdims=True)
    energy = 0.5 * totals[0:1]
    energy_ref[...] = energy
    sub8 = lax.broadcasted_iota(jnp.int32, (8, 128), 0)
    lane8 = lax.broadcasted_iota(jnp.int32, (8, 128), 1)
    full = jnp.where((sub8 >= 1) & (sub8 <= 3), energy, 0.0) - totals
    virial_ref[...] = jnp.sum(jnp.where(lane8 == sub8 - 1, full, 0.0), axis=0, keepdims=True)[:, :6]

    for h in range(2):
        many = r1.at[0, pl.ds(0, 15)]
        pltpu.make_async_copy(many, many, send1.at[h]).wait()
    for block, size in enumerate((64, 64, 64, 32, 32)):
        sent = zy.at[0, 0, pl.ds(0, 31 * size), :]
        pltpu.make_async_copy(sent, sent, send2.at[block]).wait()
    for stage in range(2):
        many = first.at[pl.ds(0, 15)]
        pltpu.make_async_copy(many, many, send3.at[stage]).wait()


def body(charges_old, spline_moduli):
    vmem, hbm = pl.BlockSpec(memory_space=pltpu.VMEM), pl.BlockSpec(memory_space=pl.ANY)
    dma = pltpu.SemaphoreType.DMA
    structure, energy, virial = pl.pallas_call(
        ewald_kernel,
        out_shape=(
            jax.ShapeDtypeStruct((2, 8, 2, 64, N), F32),
            jax.ShapeDtypeStruct((1, 1), F32),
            jax.ShapeDtypeStruct((1, 6), F32),
        ),
        in_specs=[hbm] * 4,
        out_specs=(vmem, vmem, vmem),
        scratch_shapes=[
            pltpu.SMEM((3, N), F32),
            pltpu.VMEM((3, N), F32),
            pltpu.VMEM((2, 8, 2, 32, N), F32),
            pltpu.VMEM((2, N, 640), BF16),
            pltpu.VMEM((2, 2, HALF, N), BF16),
            pltpu.VMEM((2, 2, HALF, N), BF16),
            pltpu.VMEM((4, 4, 264, 128), F32),
            pltpu.VMEM((2, 16, 264, 128), F32),
            pltpu.VMEM((2, 2, 2048, 128), F32),
            pltpu.VMEM((2, 2, 32, 64, 128), F32),
            pltpu.VMEM((7, 8, N), F32),
            pltpu.VMEM((64, N), F32),
            pltpu.VMEM((64, N), F32),
            pltpu.VMEM((8, 128), F32),
            pltpu.VMEM((16, 8, 128), F32),
            pltpu.VMEM((8, 128), F32),
            pltpu.VMEM((16, 8, 128), F32),
            dma((5,)),
            dma((2,)),
            dma((2,)),
            dma((5,)),
            dma((5,)),
            dma((2,)),
            dma((2,)),
        ],
        compiler_params=pltpu.CompilerParams(
            collective_id=0, has_side_effects=True, vmem_limit_bytes=32 * 2**20
        ),
        name="ewald",
    )(
        *[
            pltpu.with_memory_space_constraint(operand, pltpu.HBM)
            for operand in (
                spline_moduli,
                charges_old.reshape(2, 8, 2, 32, N),
                jnp.asarray(z_table()),
                jnp.asarray(half_table()),
            )
        ]
    )
    return structure.reshape(2, 16, 64, N), energy[0, 0], virial[0]


def solution(mesh):
    torus = Mesh(mesh.devices.reshape(4, 4, 2, 2, 4), AXES)
    return jax.shard_map(
        body,
        mesh=torus,
        in_specs=(P(PX, PY, None, None, None), P()),
        out_specs=(P(None, PX, PY, None), P(), P()),
        check_vma=False,
    )
```

```python
import math

import jax
import jax.numpy as jnp
import numpy as np
from jax import lax
from jax.experimental import pallas as pl
from jax.experimental.pallas import tpu as pltpu
from jax.sharding import Mesh
from jax.sharding import PartitionSpec as P

AXES = ("px_0", "px_1", "px_2", "py_0", "py_1")
PX = AXES[:3]
PY = AXES[3:]
MESH = pl.DeviceIdType.MESH
F32 = jnp.float32
BF16 = jnp.bfloat16

beta_nm = 3.12
cell_nm = 0.1
N = 512
HALF = N // 2
NT = (((1,), (1,)), ((), ()))


def split_np(a):
    hi = a.astype(BF16)
    lo = (a - hi.astype(np.float64)).astype(BF16)
    return np.stack([hi, lo])


def angles(rows, cols):
    return 2.0 * math.pi * (np.outer(rows, cols) % N) / N


def z_table():
    z = np.arange(N)
    parts = []
    for b in range(4):
        t = angles(z, 64 * b + np.arange(64))
        parts += [np.cos(t), -np.sin(t)]
    edge = np.zeros((N, 128))
    for b in range(4):
        t = angles(z, np.array([64 * (b + 1)]))[:, 0]
        edge[:, 8 * b] = np.cos(t)
        edge[:, 64 + 8 * b] = -np.sin(t)
    return split_np(np.concatenate(parts + [edge], axis=1))


def half_table():
    r = np.arange(HALF)
    out = []
    for e in range(2):
        t = angles(2 * r + e, r)
        out.append(np.concatenate([np.cos(t), np.sin(t)], axis=1))
    return split_np(np.stack(out))


def split(v):
    hi = v.astype(BF16)
    return hi, (v - hi.astype(F32)).astype(BF16)


def mm(a, b):
    return jnp.dot(a, b, preferred_element_type=F32)


def signed_wave(mode_index):
    shifted = mode_index - N * (mode_index >= HALF).astype(jnp.int32)
    return shifted.astype(F32) / (cell_nm * N)


def ewald_kernel(
    mod_hbm, x_hbm, wz_hbm, wh_hbm, out_ref, energy_ref, virial_ref,
    mod_smem, mod_ref, x_ref, wz_ref, wh_ref, zs, r1, zy, r2, acc, xz2, modxz, parts, first, middle, second,
    load, send1, recv1, send2, recv2, send3, recv3,
):
    tables = (
        (x_hbm, x_ref), (wz_hbm, wz_ref), (wh_hbm, wh_ref), (mod_hbm, mod_ref), (mod_hbm, mod_smem)
    )
    loads = [pltpu.make_async_copy(a, b, load.at[i]) for i, (a, b) in enumerate(tables)]
    for copy in loads:
        copy.start()

    yc, zh, c, lo, xc = [lax.axis_index(a) for a in AXES]
    p = yc * 8 + zh * 2 + c
    me16 = c * 8 + lo * 4 + xc
    me64 = p * 2 + lo
    outer = yc * 4 + zh
    b = xc + lo * (3 - 2 * xc)

    def peer16(t):
        d = lax.rem(me16 + t, 16)
        dc = lax.div(d, 8)
        dl = lax.rem(lax.div(d, 4), 2)
        dx = lax.rem(d, 4)
        return dc, dl, dx

    def peer64(t):
        d = lax.rem(me64 + t, 64)
        dp = lax.div(d, 2)
        dl = lax.rem(d, 2)
        dx = b + dl * (3 - 2 * b)
        return dp, dl, (lax.div(dp, 8), lax.rem(lax.div(dp, 2), 4), lax.rem(dp, 2), dl, dx)

    barrier = pltpu.get_barrier_semaphore()

    def greet16(t, carry):
        dc, dl, dx = peer16(t)
        pl.semaphore_signal(barrier, inc=1, device_id=(yc, zh, dc, dl, dx), device_id_type=MESH)
        return carry

    def greet64(t, carry):
        far = lax.rem(t + 24, 63) + 1
        pl.semaphore_signal(barrier, inc=1, device_id=peer64(far)[2], device_id_type=MESH)
        return carry

    lax.fori_loop(0, 63, greet64, 0, unroll=7)
    lax.fori_loop(1, 16, greet16, 0, unroll=5)

    narrow = lax.rem(lax.broadcasted_iota(jnp.int32, (32, 128), 1), 64) < 8

    def z_step(g, carry):
        rows = x_ref[lax.div(g, 2), :, lax.rem(g, 2)].reshape(256, N)
        hi, low = split(rows)
        out = mm(hi, wz_ref[0]) + mm(low, wz_ref[0]) + mm(hi, wz_ref[1])
        for k in range(4):
            zs[g, k, 8:264] = out[:, 128 * k : 128 * k + 128]
        edge = out[:, 512:640].reshape(8, 32, 128)
        packed = edge[0]
        for r in range(1, 8):
            packed = packed + pltpu.roll(edge[r], r, 1)
        for k in range(4):
            one = pltpu.roll(packed, 128 - 8 * k, 1) if k else packed
            one = jnp.where(narrow, one, 0.0).reshape(4, 8, 128)
            zs[g, k, 0:8] = (
                one[0]
                + pltpu.roll(one[1], 8, 1)
                + pltpu.roll(one[2], 16, 1)
                + pltpu.roll(one[3], 24, 1)
            )
        return carry

    loads[0].wait()
    loads[1].wait()
    lax.fori_loop(0, 4, z_step, 0)
    pl.semaphore_wait(barrier, 78)

    halves = (pl.ds(0, 136), pl.ds(136, 128))
    for h in range(2):

        def send_y(t, carry):
            d = lax.rem(c * 4 + xc + t, 8)
            dc, dx = lax.div(d, 4), lax.rem(d, 4)
            stay = lax.div(t, 8)
            dl = lo * stay + (1 - lo) * (1 - stay)
            pltpu.make_async_remote_copy(
                src_ref=zs.at[2 * dc + dl, dx + dl * (3 - 2 * dx), halves[h]],
                dst_ref=r1.at[me16, halves[h]],
                send_sem=send1.at[h],
                recv_sem=recv1.at[h],
                device_id=(yc, zh, dc, dl, dx),
                device_id_type=MESH,
            ).start()
            return carry

        lax.fori_loop(0, 8, send_y, 0, unroll=8)
        lax.fori_loop(9, 16, send_y, 0, unroll=7)
    r1[me16] = zs[2 * c + lo, b]

    loads[3].wait()
    loads[4].wait()
    mx = signed_wave(lax.broadcasted_iota(jnp.int32, (1, N), 1))
    mz = signed_wave(64 * (4 * lo + xc) + lax.broadcasted_iota(jnp.int32, (64, 1), 0))
    acc[...] = jnp.zeros_like(acc)
    xz2[...] = mx * mx + mz * mz
    modz = pltpu.roll(jnp.broadcast_to(mod_ref[2:3, :], (8, N)), lax.rem(N - 64 * (4 * lo + xc), N), 1)
    modz = jnp.broadcast_to(modz[0:1, :128], (128, 128)).T[:64]
    modz = jnp.concatenate([modz] * 4, axis=1)
    modxz[...] = mod_ref[0:1, :] * modz * (1.0 / (math.pi * (cell_nm * N) ** 3))

    loads[2].wait()

    lane = lax.broadcasted_iota(jnp.int32, (HALF, 128), 1)
    is_edge = (lane == 0) | (lane == 64)
    turn = jnp.where(lane < 64, 1.0, -1.0).astype(F32)

    for h in range(2):
        many = r1.at[pl.ds(0, 15), halves[h]]
        pltpu.make_async_copy(many, many, recv1.at[h]).wait()
        for e in range(2):
            base = MIRROR + 4 * (1 - e)

            def fold(first, count):
                top = r1[0:8, first : first + count]
                bottom = r1[8:16, first : first + count]
                return top + bottom if e == 0 else top - bottom

            edges = fold(0, 8)
            for r in range(4):
                i = 4 * h + r
                direct = fold(8 + 32 * i, 32).reshape(HALF, 128)
                edge = jnp.stack(
                    [pltpu.roll(edges, 128 - 8 * k - i, 2) if k + i else edges for k in range(4)],
                    axis=1,
                ).reshape(HALF, 128)
                mirror = jnp.where(is_edge, edge, direct)
                plain = jnp.concatenate([direct, mirror], axis=1)
                turned = jnp.concatenate(
                    [pltpu.roll(direct, 64, 1) * turn, pltpu.roll(mirror, 64, 1) * turn], axis=1
                )
                hi, low = split(jnp.concatenate([plain, turned], axis=0))
                out = mm(wh_ref[0, e], hi) + mm(wh_ref[1, e], hi) + mm(wh_ref[0, e], low)
                zy[e, h, pl.ds(r, HALF, stride=4), :] = out[:, :128]
                zy[e, h, pl.ds(base + r, HALF, stride=4), :] = out[:, 128:]
                if e == 0:
                    zy[e, h, pl.ds(base + 4 * HALF + r, 1), :] = out[0:1, 128:]

            def start_for(dp, dl):
                return (1 - dl) * (32 * dp) + dl * (base + 4 * (249 - e) - 32 * dp)

            r2[e, h, lo, p] = zy[e, h, pl.ds(pl.multiple_of(start_for(p, lo), 8), 32), :]
            pieces = 4 if e and h else 1
            size = 32 // pieces
            for piece in range(pieces):

                def send_x(k, turn_y):
                    part = lax.div(k + 1, 2)
                    dz = lax.rem(2 * zh + lo + 4 + part * (1 - 2 * lax.rem(k, 2)), 8)
                    dzh, dl = lax.div(dz, 2), lax.rem(dz, 2)
                    dy = lax.rem(yc + turn_y // 2, 4)
                    dc = lax.rem(c + turn_y % 2, 2)
                    dp = dy * 8 + dzh * 2 + dc
                    device = (dy, dzh, dc, dl, b + dl * (3 - 2 * b))
                    skip = size * (piece + dl * (pieces - 1 - 2 * piece))
                    start = start_for(dp, dl) + skip
                    pltpu.make_async_remote_copy(
                        src_ref=zy.at[e, h, pl.ds(pl.multiple_of(start, 8), size), :],
                        dst_ref=r2.at[e, h, lo, p, pl.ds(pl.multiple_of(skip, 8), size), :],
                        send_sem=send2.at[2 * h + e + piece],
                        recv_sem=recv2.at[2 * h + e + piece],
                        device_id=device,
                        device_id_type=MESH,
                    ).start()

                def send_plane(k, carry):
                    for i in range(8):
                        send_x(k, i)
                    return carry

                lax.fori_loop(0, 7, send_plane, 0)
                for i in range(1, 8):
                    send_x(7, i)

    flip = lo
    row = lax.broadcasted_iota(jnp.int32, (128, 128), 0)
    col = lax.broadcasted_iota(jnp.int32, (128, 128), 1)
    upper = row >= 64
    within = jnp.where(upper, row - 64, row)
    negated = jnp.where(within == 0, 0, 64 - within)
    target = jnp.where(flip == 1, negated, within) + jnp.where(upper, 64, 0)
    sign = jnp.where((flip == 1) & upper, -1.0, 1.0)
    select = jnp.where(col == target, sign, 0.0).astype(BF16)
    low_rows = lax.broadcasted_iota(jnp.int32, (32, 8, 128), 1) < 4

    def rows(v):
        return jnp.sum(v.reshape(8, 8, N), axis=0)

    for e in range(2):

        def arrived(block, size):
            many = zy.at[0, 0, pl.ds(0, 63 * size), :]
            pltpu.make_async_copy(many, many, recv2.at[block]).wait()

        arrived(e, 32)
        if e == 0:
            arrived(2, 32)

        def x_step(t, carry):
            tile = t + flip * (3 - 2 * t)

            def turned(a):
                top = r2[e, 0, a, :, pl.ds(pl.multiple_of(8 * tile, 8), 8), :]
                bottom = r2[e, 1, a, :, pl.ds(pl.multiple_of(8 * tile, 8), 8), :]
                slot0 = jnp.where(low_rows, top, pltpu.roll(bottom, 4, 1))
                slot1 = jnp.where(low_rows, pltpu.roll(top, 4, 1), bottom)
                his, lows = [], []
                for v in (jnp.where(flip == 1, slot1, slot0), jnp.where(flip == 1, slot0, slot1)):
                    hi, low = split(v.reshape(HALF, 128))
                    his.append(lax.dot_general(select, hi, NT, preferred_element_type=F32).astype(BF16))
                    lows.append(lax.dot_general(select, low, NT, preferred_element_type=F32).astype(BF16))
                hi, low = jnp.concatenate(his, axis=0), jnp.concatenate(lows, axis=0)
                return mm(hi, wh_ref[0, a]) + mm(low, wh_ref[0, a]) + mm(hi, wh_ref[1, a])

            even, odd = turned(0), turned(1)
            for j in range(2):

                def halves_of(v):
                    re, im = v[128 * j : 128 * j + 64], v[128 * j + 64 : 128 * j + 128]
                    return re[:, :HALF] + im[:, HALF:], im[:, :HALF] - re[:, HALF:]

                er, ei = halves_of(even)
                orr, oi = halves_of(odd)
                re = jnp.concatenate([er + orr, er - orr], axis=1)
                im = jnp.concatenate([ei + oi, ei - oi], axis=1)
                out_ref[0, 2 * t + j, e] = re
                out_ref[1, 2 * t + j, e] = im
                ky = 16 * p + 2 * (2 * t + j) + e
                my = (ky - jnp.where(ky >= HALF, N, 0)).astype(F32) * (1.0 / (cell_nm * N))
                mody = mod_smem[1, ky]
                msq = xz2[...] + my * my
                anchor = msq == 0.0
                inverse = 1.0 / jnp.where(anchor, 1.0, msq)
                decay = (math.pi**2 / beta_nm**2) * msq
                theta = jnp.where(anchor, 0.0, jnp.exp(-decay) * inverse * modxz[...] * mody)
                power = theta * (re * re + im * im)
                weight = power * (1.0 + decay) * inverse
                wz = weight * mz
                w0, w1, w2 = rows(weight), rows(wz), rows(wz * mz)
                acc[0] += rows(power)
                acc[1] += w0
                acc[2] += w0 * (my * my)
                acc[3] += w2
                acc[4] += w0 * my
                acc[5] += w1
                acc[6] += w1 * my
            return carry

        if e == 0:
            lax.fori_loop(0, 4, x_step, 0)
        else:
            for piece in range(4):
                arrived(3 + piece, 8)
                x_step(piece, 0)

    def lanes(v):
        v = jnp.sum(v, axis=0, keepdims=True)
        return v[:, 0:128] + v[:, 128:256] + v[:, 256:384] + v[:, 384:512]

    sub8 = lax.broadcasted_iota(jnp.int32, (8, 128), 0)
    lane8 = lax.broadcasted_iota(jnp.int32, (8, 128), 1)
    column = jnp.concatenate(
        [
            lanes(acc[0]),
            lanes(acc[1] * (mx * mx)),
            lanes(acc[2]),
            lanes(acc[3]),
            lanes(acc[4] * mx),
            lanes(acc[5] * mx),
            lanes(acc[6]),
            jnp.zeros((1, 128), F32),
        ],
        axis=0,
    )
    column = jnp.sum(column, axis=1, keepdims=True)
    parts[...] = jnp.sum(jnp.where(lane8 == sub8, column, 0.0), axis=0, keepdims=True)

    def spread(stage, source, slots, me):
        slots[me] = source[...]

        def put(t, carry):
            if stage == 0:
                dc, dl, dx = peer16(t)
                device = (yc, zh, dc, dl, dx)
            else:
                d = lax.rem(outer + t, 16)
                device = (lax.div(d, 4), lax.rem(d, 4), c, lo, xc)
            pltpu.make_async_remote_copy(
                src_ref=source,
                dst_ref=slots.at[me],
                send_sem=send3.at[stage],
                recv_sem=recv3.at[stage],
                device_id=device,
                device_id_type=MESH,
            ).start()
            return carry

        lax.fori_loop(1, 16, put, 0, unroll=5)
        many = slots.at[pl.ds(0, 15)]
        pltpu.make_async_copy(many, many, recv3.at[stage]).wait()
        return jnp.sum(slots[...], axis=0)

    middle[...] = spread(0, parts, first, me16)
    totals = jnp.broadcast_to(spread(1, middle, second, outer), (8, 128))
    energy = 0.5 * totals[:, 0:1]
    energy_ref[...] = energy[0:1]
    virial_ref[...] = (jnp.where(lane8 < 3, energy, 0.0) - pltpu.roll(totals, 127, 1))[0:1, :6]

    for h in range(2):
        many = r1.at[pl.ds(0, 15), halves[h]]
        pltpu.make_async_copy(many, many, send1.at[h]).wait()
    for block, size in enumerate((32, 32, 32, 8, 8, 8, 8)):
        sent = zy.at[0, 0, pl.ds(0, 63 * size), :]
        pltpu.make_async_copy(sent, sent, send2.at[block]).wait()
    for stage in range(2):
        many = first.at[pl.ds(0, 15)]
        pltpu.make_async_copy(many, many, send3.at[stage]).wait()


MIRROR = 1024
ROWS = 2064


def body(charges_old, spline_moduli):
    vmem, hbm = pl.BlockSpec(memory_space=pltpu.VMEM), pl.BlockSpec(memory_space=pl.ANY)
    dma = pltpu.SemaphoreType.DMA
    structure, energy, virial = pl.pallas_call(
        ewald_kernel,
        out_shape=(
            jax.ShapeDtypeStruct((2, 8, 2, 64, N), F32),
            jax.ShapeDtypeStruct((1, 1), F32),
            jax.ShapeDtypeStruct((1, 6), F32),
        ),
        in_specs=[hbm] * 4,
        out_specs=(vmem, vmem, vmem),
        scratch_shapes=[
            pltpu.SMEM((3, N), F32),
            pltpu.VMEM((3, N), F32),
            pltpu.VMEM((2, 8, 2, 32, N), F32),
            pltpu.VMEM((2, N, 640), BF16),
            pltpu.VMEM((2, 2, HALF, N), BF16),
            pltpu.VMEM((4, 4, 264, 128), F32),
            pltpu.VMEM((16, 264, 128), F32),
            pltpu.VMEM((2, 2, ROWS, 128), F32),
            pltpu.VMEM((2, 2, 2, 32, 32, 128), F32),
            pltpu.VMEM((7, 8, N), F32),
            pltpu.VMEM((64, N), F32),
            pltpu.VMEM((64, N), F32),
            pltpu.VMEM((1, 128), F32),
            pltpu.VMEM((16, 1, 128), F32),
            pltpu.VMEM((1, 128), F32),
            pltpu.VMEM((16, 1, 128), F32),
            dma((5,)),
            dma((2,)),
            dma((2,)),
            dma((7,)),
            dma((7,)),
            dma((2,)),
            dma((2,)),
        ],
        compiler_params=pltpu.CompilerParams(
            collective_id=0, has_side_effects=True, vmem_limit_bytes=24 * 2**20
        ),
        name="ewald",
    )(
        *[
            pltpu.with_memory_space_constraint(operand, pltpu.HBM)
            for operand in (
                spline_moduli,
                charges_old.reshape(2, 8, 2, 32, N),
                jnp.asarray(z_table()),
                jnp.asarray(half_table()),
            )
        ]
    )
    return structure.reshape(2, 16, 64, N), energy[0, 0], virial[0]


def solution(mesh):
    torus = Mesh(mesh.devices.reshape(4, 4, 2, 2, 4), AXES)
    return jax.shard_map(
        body,
        mesh=torus,
        in_specs=(P(PX, PY, None, None, None), P()),
        out_specs=(P(None, PX, PY, None), P(), P()),
        check_vma=False,
    )
```

```python
import math

import jax
import jax.numpy as jnp
import numpy as np
from jax import lax
from jax.experimental import pallas as pl
from jax.experimental.pallas import tpu as pltpu
from jax.sharding import Mesh
from jax.sharding import PartitionSpec as P

AXES = ("px_0", "px_1", "px_2", "py_0", "py_1")
PX = AXES[:3]
PY = AXES[3:]
MESH = pl.DeviceIdType.MESH
F32 = jnp.float32
BF16 = jnp.bfloat16

beta_nm = 3.12
cell_nm = 0.1
N = 512
HALF = N // 2
NT = (((1,), (1,)), ((), ()))


def split_np(a):
    hi = a.astype(BF16)
    lo = (a - hi.astype(np.float64)).astype(BF16)
    return np.stack([hi, lo])


def angles(rows, cols):
    return 2.0 * math.pi * (np.outer(rows, cols) % N) / N


def z_table():
    z = np.arange(N)
    parts = []
    for b in range(4):
        t = angles(z, 64 * b + np.arange(64))
        parts += [np.cos(t), -np.sin(t)]
    edge = np.zeros((N, 128))
    for b in range(4):
        t = angles(z, np.array([64 * (b + 1)]))[:, 0]
        edge[:, 8 * b] = np.cos(t)
        edge[:, 64 + 8 * b] = -np.sin(t)
    return split_np(np.concatenate(parts + [edge], axis=1))


def half_table():
    r = np.arange(HALF)
    out = []
    for e in range(2):
        t = angles(2 * r + e, r)
        out.append(np.concatenate([np.cos(t), np.sin(t)], axis=1))
    return split_np(np.stack(out))


def split(v):
    hi = v.astype(BF16)
    return hi, (v - hi.astype(F32)).astype(BF16)


def mm(a, b):
    return jnp.dot(a, b, preferred_element_type=F32)


def signed_wave(mode_index):
    shifted = mode_index - N * (mode_index >= HALF).astype(jnp.int32)
    return shifted.astype(F32) / (cell_nm * N)


def ewald_kernel(
    mod_hbm, x_hbm, wz_hbm, wh_hbm, out_ref, energy_ref, virial_ref,
    mod_smem, mod_ref, x_ref, wz_ref, wh_ref, zs, r1, zy, r2, acc, xz2, modxz, parts, first, middle, second,
    load, send1, recv1, send2, recv2, send3, recv3,
):
    tables = [(wz_hbm, wz_ref)]
    tables += [(x_hbm.at[g // 2, :, g % 2], x_ref.at[g // 2, :, g % 2]) for g in range(4)]
    tables += [(wh_hbm, wh_ref), (mod_hbm, mod_ref), (mod_hbm, mod_smem)]
    loads = [pltpu.make_async_copy(a, b, load.at[i]) for i, (a, b) in enumerate(tables)]
    for copy in loads:
        copy.start()

    yc, zh, c, lo, xc = [lax.axis_index(a) for a in AXES]
    p = yc * 8 + zh * 2 + c
    me16 = c * 8 + lo * 4 + xc
    me64 = p * 2 + lo
    outer = yc * 4 + zh
    b = xc + lo * (3 - 2 * xc)

    def peer16(t):
        d = lax.rem(me16 + t, 16)
        dc = lax.div(d, 8)
        dl = lax.rem(lax.div(d, 4), 2)
        dx = lax.rem(d, 4)
        return dc, dl, dx

    def peer64(t):
        d = lax.rem(me64 + t, 64)
        dp = lax.div(d, 2)
        dl = lax.rem(d, 2)
        dx = b + dl * (3 - 2 * b)
        return dp, dl, (lax.div(dp, 8), lax.rem(lax.div(dp, 2), 4), lax.rem(dp, 2), dl, dx)

    barrier = pltpu.get_barrier_semaphore()

    def greet16(t, carry):
        dc, dl, dx = peer16(t)
        pl.semaphore_signal(barrier, inc=1, device_id=(yc, zh, dc, dl, dx), device_id_type=MESH)
        return carry

    def greet64(t, carry):
        far = lax.rem(t + 24, 63) + 1
        pl.semaphore_signal(barrier, inc=1, device_id=peer64(far)[2], device_id_type=MESH)
        return carry

    lax.fori_loop(0, 63, greet64, 0, unroll=7)
    lax.fori_loop(1, 16, greet16, 0, unroll=5)

    narrow = lax.rem(lax.broadcasted_iota(jnp.int32, (32, 128), 1), 64) < 8

    def z_step(g, carry):
        rows = x_ref[g // 2, :, g % 2].reshape(256, N)
        hi, low = split(rows)
        out = mm(hi, wz_ref[0]) + mm(low, wz_ref[0]) + mm(hi, wz_ref[1])
        for k in range(4):
            zs[g, k, 8:264] = out[:, 128 * k : 128 * k + 128]
        edge = out[:, 512:640].reshape(8, 32, 128)
        packed = edge[0]
        for r in range(1, 8):
            packed = packed + pltpu.roll(edge[r], r, 1)
        for k in range(4):
            one = pltpu.roll(packed, 128 - 8 * k, 1) if k else packed
            one = jnp.where(narrow, one, 0.0).reshape(4, 8, 128)
            zs[g, k, 0:8] = (
                one[0]
                + pltpu.roll(one[1], 8, 1)
                + pltpu.roll(one[2], 16, 1)
                + pltpu.roll(one[3], 24, 1)
            )
        return carry

    loads[0].wait()
    for g in range(4):
        loads[1 + g].wait()
        z_step(g, 0)
    pl.semaphore_wait(barrier, 78)

    halves = (pl.ds(0, 136), pl.ds(136, 128))
    for h in range(2):

        def send_y(t, carry):
            d = lax.rem(c * 4 + xc + t, 8)
            dc, dx = lax.div(d, 4), lax.rem(d, 4)
            stay = lax.div(t, 8)
            dl = lo * stay + (1 - lo) * (1 - stay)
            pltpu.make_async_remote_copy(
                src_ref=zs.at[2 * dc + dl, dx + dl * (3 - 2 * dx), halves[h]],
                dst_ref=r1.at[me16, halves[h]],
                send_sem=send1.at[h],
                recv_sem=recv1.at[h],
                device_id=(yc, zh, dc, dl, dx),
                device_id_type=MESH,
            ).start()
            return carry

        lax.fori_loop(0, 8, send_y, 0, unroll=8)
        lax.fori_loop(9, 16, send_y, 0, unroll=7)
    r1[me16] = zs[2 * c + lo, b]

    loads[6].wait()
    loads[7].wait()
    mx = signed_wave(lax.broadcasted_iota(jnp.int32, (1, N), 1))
    mz = signed_wave(64 * (4 * lo + xc) + lax.broadcasted_iota(jnp.int32, (64, 1), 0))
    acc[...] = jnp.zeros_like(acc)
    xz2[...] = mx * mx + mz * mz
    modz = pltpu.roll(jnp.broadcast_to(mod_ref[2:3, :], (8, N)), lax.rem(N - 64 * (4 * lo + xc), N), 1)
    modz = jnp.broadcast_to(modz[0:1, :128], (128, 128)).T[:64]
    modz = jnp.concatenate([modz] * 4, axis=1)
    modxz[...] = mod_ref[0:1, :] * modz * (1.0 / (math.pi * (cell_nm * N) ** 3))

    loads[5].wait()

    lane = lax.broadcasted_iota(jnp.int32, (HALF, 128), 1)
    is_edge = (lane == 0) | (lane == 64)
    turn = jnp.where(lane < 64, 1.0, -1.0).astype(F32)

    for h in range(2):
        many = r1.at[pl.ds(0, 15), halves[h]]
        pltpu.make_async_copy(many, many, recv1.at[h]).wait()
        for e in range(2):
            base = MIRROR + 4 * (1 - e)

            def fold(first, count):
                top = r1[0:8, first : first + count]
                bottom = r1[8:16, first : first + count]
                return top + bottom if e == 0 else top - bottom

            edges = fold(0, 8)
            for r in range(4):
                i = 4 * h + r
                direct = fold(8 + 32 * i, 32).reshape(HALF, 128)
                edge = jnp.stack(
                    [pltpu.roll(edges, 128 - 8 * k - i, 2) if k + i else edges for k in range(4)],
                    axis=1,
                ).reshape(HALF, 128)
                mirror = jnp.where(is_edge, edge, direct)
                plain = jnp.concatenate([direct, mirror], axis=1)
                turned = jnp.concatenate(
                    [pltpu.roll(direct, 64, 1) * turn, pltpu.roll(mirror, 64, 1) * turn], axis=1
                )
                hi, low = split(jnp.concatenate([plain, turned], axis=0))
                out = mm(wh_ref[0, e], hi) + mm(wh_ref[1, e], hi) + mm(wh_ref[0, e], low)
                zy[e, h, pl.ds(r, HALF, stride=4), :] = out[:, :128]
                zy[e, h, pl.ds(base + r, HALF, stride=4), :] = out[:, 128:]
                if e == 0:
                    zy[e, h, pl.ds(base + 4 * HALF + r, 1), :] = out[0:1, 128:]

            def start_for(dp, dl):
                return (1 - dl) * (32 * dp) + dl * (base + 4 * (249 - e) - 32 * dp)

            r2[e, h, lo, p] = zy[e, h, pl.ds(pl.multiple_of(start_for(p, lo), 8), 32), :]
            pieces = 4 if e and h else 1
            size = 32 // pieces
            for piece in range(pieces):

                def send_x(k, turn_y):
                    part = lax.div(k + 1, 2)
                    dz = lax.rem(2 * zh + lo + 4 + part * (1 - 2 * lax.rem(k, 2)), 8)
                    dzh, dl = lax.div(dz, 2), lax.rem(dz, 2)
                    dy = lax.rem(yc + turn_y // 2, 4)
                    dc = lax.rem(c + turn_y % 2, 2)
                    dp = dy * 8 + dzh * 2 + dc
                    device = (dy, dzh, dc, dl, b + dl * (3 - 2 * b))
                    skip = size * (piece + dl * (pieces - 1 - 2 * piece))
                    start = start_for(dp, dl) + skip
                    pltpu.make_async_remote_copy(
                        src_ref=zy.at[e, h, pl.ds(pl.multiple_of(start, 8), size), :],
                        dst_ref=r2.at[e, h, lo, p, pl.ds(pl.multiple_of(skip, 8), size), :],
                        send_sem=send2.at[2 * h + e + piece],
                        recv_sem=recv2.at[2 * h + e + piece],
                        device_id=device,
                        device_id_type=MESH,
                    ).start()

                def send_plane(k, carry):
                    for i in range(8):
                        send_x(k, i)
                    return carry

                lax.fori_loop(0, 7, send_plane, 0)
                for i in range(1, 8):
                    send_x(7, i)

    flip = lo
    row = lax.broadcasted_iota(jnp.int32, (128, 128), 0)
    col = lax.broadcasted_iota(jnp.int32, (128, 128), 1)
    upper = row >= 64
    within = jnp.where(upper, row - 64, row)
    negated = jnp.where(within == 0, 0, 64 - within)
    target = jnp.where(flip == 1, negated, within) + jnp.where(upper, 64, 0)
    sign = jnp.where((flip == 1) & upper, -1.0, 1.0)
    select = jnp.where(col == target, sign, 0.0).astype(BF16)
    low_rows = lax.broadcasted_iota(jnp.int32, (32, 8, 128), 1) < 4

    def rows(v):
        return jnp.sum(v.reshape(8, 8, N), axis=0)

    for e in range(2):

        def arrived(block, size):
            many = zy.at[0, 0, pl.ds(0, 63 * size), :]
            pltpu.make_async_copy(many, many, recv2.at[block]).wait()

        arrived(e, 32)
        if e == 0:
            arrived(2, 32)

        def x_step(t, carry):
            tile = t + flip * (3 - 2 * t)

            def turned(a):
                top = r2[e, 0, a, :, pl.ds(pl.multiple_of(8 * tile, 8), 8), :]
                bottom = r2[e, 1, a, :, pl.ds(pl.multiple_of(8 * tile, 8), 8), :]
                slot0 = jnp.where(low_rows, top, pltpu.roll(bottom, 4, 1))
                slot1 = jnp.where(low_rows, pltpu.roll(top, 4, 1), bottom)
                his, lows = [], []
                for v in (jnp.where(flip == 1, slot1, slot0), jnp.where(flip == 1, slot0, slot1)):
                    hi, low = split(v.reshape(HALF, 128))
                    his.append(lax.dot_general(select, hi, NT, preferred_element_type=F32).astype(BF16))
                    lows.append(lax.dot_general(select, low, NT, preferred_element_type=F32).astype(BF16))
                hi, low = jnp.concatenate(his, axis=0), jnp.concatenate(lows, axis=0)
                return mm(hi, wh_ref[0, a]) + mm(low, wh_ref[0, a]) + mm(hi, wh_ref[1, a])

            even, odd = turned(0), turned(1)
            for j in range(2):

                def halves_of(v):
                    re, im = v[128 * j : 128 * j + 64], v[128 * j + 64 : 128 * j + 128]
                    return re[:, :HALF] + im[:, HALF:], im[:, :HALF] - re[:, HALF:]

                er, ei = halves_of(even)
                orr, oi = halves_of(odd)
                re = jnp.concatenate([er + orr, er - orr], axis=1)
                im = jnp.concatenate([ei + oi, ei - oi], axis=1)
                out_ref[0, 2 * t + j, e] = re
                out_ref[1, 2 * t + j, e] = im
                ky = 16 * p + 2 * (2 * t + j) + e
                my = (ky - jnp.where(ky >= HALF, N, 0)).astype(F32) * (1.0 / (cell_nm * N))
                mody = mod_smem[1, ky]
                msq = xz2[...] + my * my
                anchor = msq == 0.0
                inverse = 1.0 / jnp.where(anchor, 1.0, msq)
                decay = (math.pi**2 / beta_nm**2) * msq
                theta = jnp.where(anchor, 0.0, jnp.exp(-decay) * inverse * modxz[...] * mody)
                power = theta * (re * re + im * im)
                weight = power * (1.0 + decay) * inverse
                wz = weight * mz
                w0, w1, w2 = rows(weight), rows(wz), rows(wz * mz)
                acc[0] += rows(power)
                acc[1] += w0
                acc[2] += w0 * (my * my)
                acc[3] += w2
                acc[4] += w0 * my
                acc[5] += w1
                acc[6] += w1 * my
            return carry

        if e == 0:
            lax.fori_loop(0, 4, x_step, 0)
        else:
            for piece in range(4):
                arrived(3 + piece, 8)
                x_step(piece, 0)

    def lanes(v):
        v = jnp.sum(v, axis=0, keepdims=True)
        return v[:, 0:128] + v[:, 128:256] + v[:, 256:384] + v[:, 384:512]

    sub8 = lax.broadcasted_iota(jnp.int32, (8, 128), 0)
    lane8 = lax.broadcasted_iota(jnp.int32, (8, 128), 1)
    column = jnp.concatenate(
        [
            lanes(acc[0]),
            lanes(acc[1] * (mx * mx)),
            lanes(acc[2]),
            lanes(acc[3]),
            lanes(acc[4] * mx),
            lanes(acc[5] * mx),
            lanes(acc[6]),
            jnp.zeros((1, 128), F32),
        ],
        axis=0,
    )
    column = jnp.sum(column, axis=1, keepdims=True)
    parts[...] = jnp.sum(jnp.where(lane8 == sub8, column, 0.0), axis=0, keepdims=True)

    def spread(stage, source, slots, me):
        slots[me] = source[...]

        def put(t, carry):
            if stage == 0:
                dc, dl, dx = peer16(t)
                device = (yc, zh, dc, dl, dx)
            else:
                d = lax.rem(outer + t, 16)
                device = (lax.div(d, 4), lax.rem(d, 4), c, lo, xc)
            pltpu.make_async_remote_copy(
                src_ref=source,
                dst_ref=slots.at[me],
                send_sem=send3.at[stage],
                recv_sem=recv3.at[stage],
                device_id=device,
                device_id_type=MESH,
            ).start()
            return carry

        lax.fori_loop(1, 16, put, 0, unroll=5)
        many = slots.at[pl.ds(0, 15)]
        pltpu.make_async_copy(many, many, recv3.at[stage]).wait()
        return jnp.sum(slots[...], axis=0)

    middle[...] = spread(0, parts, first, me16)
    totals = jnp.broadcast_to(spread(1, middle, second, outer), (8, 128))
    energy = 0.5 * totals[:, 0:1]
    energy_ref[...] = energy[0:1]
    virial_ref[...] = (jnp.where(lane8 < 3, energy, 0.0) - pltpu.roll(totals, 127, 1))[0:1, :6]

    for h in range(2):
        many = r1.at[pl.ds(0, 15), halves[h]]
        pltpu.make_async_copy(many, many, send1.at[h]).wait()
    for block, size in enumerate((32, 32, 32, 8, 8, 8, 8)):
        sent = zy.at[0, 0, pl.ds(0, 63 * size), :]
        pltpu.make_async_copy(sent, sent, send2.at[block]).wait()
    for stage in range(2):
        many = first.at[pl.ds(0, 15)]
        pltpu.make_async_copy(many, many, send3.at[stage]).wait()


MIRROR = 1024
ROWS = 2064


def body(charges_old, spline_moduli):
    vmem, hbm = pl.BlockSpec(memory_space=pltpu.VMEM), pl.BlockSpec(memory_space=pl.ANY)
    dma = pltpu.SemaphoreType.DMA
    structure, energy, virial = pl.pallas_call(
        ewald_kernel,
        out_shape=(
            jax.ShapeDtypeStruct((2, 8, 2, 64, N), F32),
            jax.ShapeDtypeStruct((1, 1), F32),
            jax.ShapeDtypeStruct((1, 6), F32),
        ),
        in_specs=[hbm] * 4,
        out_specs=(vmem, vmem, vmem),
        scratch_shapes=[
            pltpu.SMEM((3, N), F32),
            pltpu.VMEM((3, N), F32),
            pltpu.VMEM((2, 8, 2, 32, N), F32),
            pltpu.VMEM((2, N, 640), BF16),
            pltpu.VMEM((2, 2, HALF, N), BF16),
            pltpu.VMEM((4, 4, 264, 128), F32),
            pltpu.VMEM((16, 264, 128), F32),
            pltpu.VMEM((2, 2, ROWS, 128), F32),
            pltpu.VMEM((2, 2, 2, 32, 32, 128), F32),
            pltpu.VMEM((7, 8, N), F32),
            pltpu.VMEM((64, N), F32),
            pltpu.VMEM((64, N), F32),
            pltpu.VMEM((1, 128), F32),
            pltpu.VMEM((16, 1, 128), F32),
            pltpu.VMEM((1, 128), F32),
            pltpu.VMEM((16, 1, 128), F32),
            dma((8,)),
            dma((2,)),
            dma((2,)),
            dma((7,)),
            dma((7,)),
            dma((2,)),
            dma((2,)),
        ],
        compiler_params=pltpu.CompilerParams(
            collective_id=0, has_side_effects=True, vmem_limit_bytes=24 * 2**20
        ),
        name="ewald",
    )(
        *[
            pltpu.with_memory_space_constraint(operand, pltpu.HBM)
            for operand in (
                spline_moduli,
                charges_old.reshape(2, 8, 2, 32, N),
                jnp.asarray(z_table()),
                jnp.asarray(half_table()),
            )
        ]
    )
    return structure.reshape(2, 16, 64, N), energy[0, 0], virial[0]


def solution(mesh):
    torus = Mesh(mesh.devices.reshape(4, 4, 2, 2, 4), AXES)
    return jax.shard_map(
        body,
        mesh=torus,
        in_specs=(P(PX, PY, None, None, None), P()),
        out_specs=(P(None, PX, PY, None), P(), P()),
        check_vma=False,
    )
```
